32 devices in a mesh: dp: 2 (over x), ctx: 16 (over z, y, core).
Axes of the slice: x: 2, y: 2, z: 4, core: 2. Of those that a mesh axis runs over, the one named last changes fastest.
Arguments:
- patches: bfloat16 [2, 1024, 1280], P('dp', 'ctx'), may hold values from -6 to 6
- vit_norm_gain: float32 [1280], replicated, may hold values from 0.1 to 1.9
- vit_qkv: bfloat16 [1280, 1920], P('dp'), may hold values from -0.15625 to 0.15625
- vit_out: bfloat16 [640, 1280], P('dp'), may hold values from -0.25 to 0.25
- merger: bfloat16 [5120, 8192], P('dp', 'ctx'), may hold values from -0.078125 to 0.078125
- text_embed: bfloat16 [2, 2048, 8192], P('dp', 'ctx'), may hold values from -6 to 6
- lang_norm_gain: float32 [8192], replicated, may hold values from 0.1 to 1.9
- key_weight: bfloat16 [8192, 512], P('dp'), may hold values from -0.0625 to 0.0625
- key_cotangent: bfloat16 [2, 2048, 512], P('dp', 'ctx'), may hold values from -6 to 6
- image_grid: int32 [2, 16, 2], P('dp'), may hold values from 1 to 16, as said below
- image_start: int32 [2, 16], P('dp'), may hold values from 0 to 2047, as said below
Outputs:
- key_rot: bfloat16 [2, 2048, 512], P('dp', 'ctx')
- merger_grad: float32 [5120, 8192], P('dp', 'ctx')
The draws below stay inside these ranges and needn't reach their ends.
Inputs may be any that keep to these rules, and one draw needn't show every extreme that they name: `image_grid`: the image held by device c of ctx has a grid of rows by columns merged tokens with rows times columns at most 16, equal to 16 for some device of every sequence. Its 4 * rows * columns patches are the first rows of that device's patch block, each 2x2 merge window as 4 consecutive rows, windows in row-major order; the remaining rows are unused. `image_start`: the image occupies rows * columns consecutive positions from here. The range of 128 positions of each device along ctx holds exactly one image, wholly.
All inputs are finite; a program needn't handle non-finite values.
Results may differ from the reference program's by a relative error of at most 0.015.
Values may be sent and summed in bfloat16 or wider, within the bound.
No kernel may reach another device: no remote copies, remote signals or barrier semaphores. Data moves between devices by JAX's collectives and lax.ppermute only.
A program may use at most 128 MiB of HBM per device.

```python
import math
import jax
import jax.numpy as jnp
from jax import lax

D = 8192
VW = 1280
VHD = 80
HD = 128
TOK_DEV = 128
CAPM = 16
SEQS = 2
LENGTH = 2048
VATT = 640
MERGE_IN = 5120
KW = 512
N_CTX = 16


def permute_one(order_key):
    return jax.random.permutation(order_key, N_CTX)


def image_layout(key):
    base_key = jax.random.fold_in(key, 7321)
    key_rows, key_cols, key_full, key_order, key_offset = jax.random.split(base_key, 5)
    grid_rows = jax.random.randint(key_rows, (SEQS, N_CTX), 1, CAPM + 1)
    raw_cols = jax.random.randint(key_cols, (SEQS, N_CTX), 0, 1 << 20)
    grid_cols = 1 + raw_cols % (CAPM // grid_rows)
    forced = jax.random.randint(key_full, (SEQS, 1), 0, N_CTX)
    owner_index = jnp.arange(N_CTX)[None, :]
    grid_rows = jnp.where(owner_index == forced, 1, grid_rows)
    grid_cols = jnp.where(owner_index == forced, CAPM, grid_cols)
    counts = grid_rows * grid_cols
    order_keys = jax.random.split(key_order, SEQS)
    ranges = jax.vmap(permute_one)(order_keys)
    raw_offset = jax.random.randint(key_offset, (SEQS, N_CTX), 0, 1 << 20)
    offsets = raw_offset % (TOK_DEV - counts + 1)
    starts = ranges * TOK_DEV + offsets
    grids = jnp.stack([grid_rows, grid_cols], axis=-1)
    return (grids.astype(jnp.int32), starts.astype(jnp.int32))


def draw_image_grid(key, part):
    return image_layout(key)[0]


def draw_image_start(key, part):
    return image_layout(key)[1]


def block_scale(rng, shape, pieces, low, top_value):
    level = 1.0
    for position, shards_of in pieces:
        heights = jax.random.uniform(jax.random.fold_in(jax.random.fold_in(rng, 6), position), (shards_of,), jnp.float32, low / len(pieces), top_value / len(pieces))
        level = level * jnp.repeat(jnp.exp(heights), shape[position] // shards_of).reshape((-1,) + (1,) * (len(shape) - 1 - position))
    return level


def noise(rng, shape, spread, limit, cuts=(), kind=jnp.bfloat16):
    level = block_scale(rng, shape, cuts, -0.22, 0.18) if cuts else 1.0
    entries = jax.random.normal(rng, shape, jnp.float32) * spread * level
    return jnp.minimum(jnp.maximum(entries, -limit), limit).astype(kind)


def setup_inputs(seed: int = 0) -> dict:
    arg_keys = jax.random.split(jax.random.key(seed), 12)
    patches = noise(arg_keys[0], (SEQS, N_CTX * 4 * CAPM, VW), 1.0, 6.0, ((0, 2), (1, 16)))
    vit_norm_gain = jnp.clip(1.0 + 0.18 * jax.random.normal(arg_keys[1], (VW,), jnp.float32), 0.1, 1.9)
    vit_qkv = noise(arg_keys[2], (VW, 3 * VATT), VW ** -0.5, 0.15625, ((0, 2),))
    vit_out = noise(arg_keys[3], (VATT, VW), VATT ** -0.5, 0.25, ((0, 2),))
    merger = noise(arg_keys[4], (MERGE_IN, D), MERGE_IN ** -0.5, 0.078125, ((0, 2), (1, 16)))
    text_embed = noise(arg_keys[5], (SEQS, LENGTH, D), 1.0, 6.0, ((0, 2), (1, 16)))
    lang_norm_gain = jnp.clip(1.0 + 0.18 * jax.random.normal(arg_keys[6], (D,), jnp.float32), 0.1, 1.9)
    key_weight = noise(arg_keys[7], (D, KW), D ** -0.5, 0.0625, ((0, 2),))
    key_cotangent = noise(arg_keys[8], (SEQS, LENGTH, KW), 1.0, 6.0, ((0, 2), (1, 16)))
    image_grid = draw_image_grid(jax.random.fold_in(arg_keys[11], 71), 0)
    image_start = draw_image_start(jax.random.fold_in(arg_keys[11], 71), 0)
    return dict(patches=patches, vit_norm_gain=vit_norm_gain, vit_qkv=vit_qkv, vit_out=vit_out, merger=merger, text_embed=text_embed, lang_norm_gain=lang_norm_gain, key_weight=key_weight, key_cotangent=key_cotangent, image_grid=image_grid, image_start=image_start)


EPS = 1e-06
THETA = 1000000.0

def layer_norm(values):
    average = lax.optimization_barrier(jnp.mean(values, axis=-1, keepdims=True))
    centered = values - average
    variance = lax.optimization_barrier(jnp.mean(centered * centered, axis=-1, keepdims=True))
    return centered * lax.rsqrt(variance + EPS)

def vision_image(patch_rows, count, norm_gain, qkv_weight, out_weight):
    values = patch_rows.astype(jnp.float32)
    normed = (layer_norm(values) * norm_gain).astype(jnp.bfloat16)
    projected = jnp.dot(normed, qkv_weight, preferred_element_type=jnp.float32).astype(jnp.bfloat16)
    width = qkv_weight.shape[1] // 3
    head_count = width // VHD
    queries = projected[:, :width].reshape(-1, head_count, VHD).astype(jnp.float32)
    key_vecs = projected[:, width:2 * width].reshape(-1, head_count, VHD).astype(jnp.float32)
    value_vecs = projected[:, 2 * width:].reshape(-1, head_count, VHD).astype(jnp.float32)
    scores = jnp.einsum('qhd,khd->hqk', queries, key_vecs) / math.sqrt(VHD)
    alive_mask = (jnp.arange(values.shape[0], dtype=jnp.int32) < 4 * count).astype(jnp.float32)
    weights = jnp.exp(scores) * alive_mask[None, None, :]
    probability = (weights / lax.optimization_barrier(jnp.sum(weights, axis=-1, keepdims=True))).astype(jnp.bfloat16)
    attended = jnp.einsum('hqk,khd->qhd', probability.astype(jnp.float32), value_vecs)
    attended = attended.reshape(values.shape[0], width).astype(jnp.bfloat16)
    vit_hidden = values + jnp.dot(attended, out_weight, preferred_element_type=jnp.float32)
    merged = layer_norm(vit_hidden).astype(jnp.bfloat16).reshape(-1, 4 * values.shape[1])
    keeping = jnp.arange(merged.shape[0], dtype=jnp.int32) < count
    return jnp.where(keeping[:, None], merged, jnp.zeros_like(merged))

def rope_tables(pos_t, pos_h, pos_w):
    half_dim = HD // 2
    freq_index = jnp.arange(half_dim, dtype=jnp.int32)
    inverse = THETA ** (-(2.0 * freq_index.astype(jnp.float32)) / HD)
    first_cut = HD // 8
    second_cut = first_cut + 3 * HD // 16
    chosen = jnp.where(freq_index[None, :] < first_cut, pos_t[:, None], jnp.where(freq_index[None, :] < second_cut, pos_h[:, None], pos_w[:, None]))
    angles = chosen.astype(jnp.float32) * inverse[None, :]
    return (jnp.cos(angles), jnp.sin(angles))

def rotate(vectors, cosine, sines):
    half_dim = vectors.shape[-1] // 2
    first_half = vectors[..., :half_dim]
    second_half = vectors[..., half_dim:]
    cos_part = cosine[:, None, :]
    sin_part = sines[:, None, :]
    return jnp.concatenate([first_half * cos_part - second_half * sin_part, second_half * cos_part + first_half * sin_part], axis=-1)

def unrotate(vectors, cosine, sines):
    half_dim = vectors.shape[-1] // 2
    first_half = vectors[..., :half_dim]
    second_half = vectors[..., half_dim:]
    cos_part = cosine[:, None, :]
    sin_part = sines[:, None, :]
    return jnp.concatenate([first_half * cos_part + second_half * sin_part, second_half * cos_part - first_half * sin_part], axis=-1)

def norm_backward(rows, grad_rows, gain):
    values = rows.astype(jnp.float32)
    row_scale = lax.rsqrt(lax.optimization_barrier(jnp.mean(values * values, axis=-1, keepdims=True)) + EPS)
    weighted = grad_rows * gain
    return row_scale * weighted - values * row_scale ** 3 * lax.optimization_barrier(jnp.mean(values * weighted, axis=-1, keepdims=True))

def reference(patches, vit_norm_gain, vit_qkv, vit_out, merger, text_embed, lang_norm_gain, key_weight, key_cotangent, image_grid, image_start):
    length = text_embed.shape[1]
    head_count = key_weight.shape[1] // HD

    def one_sequence(running, inputs):
        patch_rows, text_rows, cotangent, grid_sizes, start_pos = inputs
        grid_rows = grid_sizes[:, 0]
        grid_cols = grid_sizes[:, 1]
        counts = grid_rows * grid_cols
        owned = patch_rows.reshape(N_CTX, 4 * CAPM, VW)
        merged = jax.vmap(vision_image, in_axes=(0, 0, None, None, None))(owned, counts, vit_norm_gain, vit_qkv, vit_out)
        flat = merged.reshape(N_CTX * CAPM, -1)
        embedded = jnp.dot(flat, merger, preferred_element_type=jnp.float32).astype(jnp.bfloat16)
        slot_index = jnp.arange(CAPM, dtype=jnp.int32)
        alive = slot_index[None, :] < counts[:, None]
        target = jnp.where(alive, start_pos[:, None] + slot_index[None, :], length).reshape(-1).astype(jnp.int32)
        hidden = text_rows.at[target].set(embedded, mode='drop')
        base_pos = jnp.arange(length, dtype=jnp.int32)
        image_t = jnp.repeat(start_pos, CAPM).astype(jnp.int32)
        image_h = (start_pos[:, None] + slot_index[None, :] // grid_cols[:, None]).reshape(-1).astype(jnp.int32)
        image_w = (start_pos[:, None] + slot_index[None, :] % grid_cols[:, None]).reshape(-1).astype(jnp.int32)
        pos_t = base_pos.at[target].set(image_t, mode='drop')
        pos_h = base_pos.at[target].set(image_h, mode='drop')
        pos_w = base_pos.at[target].set(image_w, mode='drop')
        hidden_float = hidden.astype(jnp.float32)
        row_scale = lax.rsqrt(lax.optimization_barrier(jnp.mean(hidden_float * hidden_float, axis=-1, keepdims=True)) + EPS)
        normed = (hidden_float * row_scale * lang_norm_gain).astype(jnp.bfloat16)
        key_proj = jnp.dot(normed, key_weight, preferred_element_type=jnp.float32)
        cosine, sines = rope_tables(pos_t, pos_h, pos_w)
        rotated = rotate(key_proj.reshape(length, head_count, HD), cosine, sines).reshape(length, -1).astype(jnp.bfloat16)
        grad_key = unrotate(cotangent.astype(jnp.float32).reshape(length, head_count, HD), cosine, sines).reshape(length, -1)
        picked = jnp.take(grad_key, jnp.minimum(target, length - 1), axis=0).astype(jnp.bfloat16)
        grad_normed = jnp.dot(picked, key_weight.T, preferred_element_type=jnp.float32)
        grad_hidden = norm_backward(embedded, grad_normed, lang_norm_gain)
        grad_embedded = jnp.where(alive.reshape(-1)[:, None], grad_hidden, 0.0).astype(jnp.bfloat16)
        term = jnp.dot(flat.T, grad_embedded, preferred_element_type=jnp.float32).astype(jnp.bfloat16)
        running = running + lax.optimization_barrier(term).astype(jnp.float32)
        return (running, rotated)
    initial = jnp.zeros(merger.shape, jnp.float32)
    merger_grad, key_rot = lax.scan(one_sequence, initial, (patches, text_embed, key_cotangent, image_grid, image_start))
    return (key_rot, merger_grad)
```

```python
import math

import jax
import jax.numpy as jnp
from jax import lax
from jax.sharding import PartitionSpec as P

VHD = 80
HD = 128
EPS = 1e-06
THETA = 1000000.0
HIGHEST = lax.Precision.HIGHEST
BF16 = jnp.bfloat16
F32 = jnp.float32


def layer_norm(values):
    average = jnp.mean(values, axis=-1, keepdims=True)
    centered = values - average
    variance = jnp.mean(centered * centered, axis=-1, keepdims=True)
    return centered * lax.rsqrt(variance + EPS)


def dot(a, b, **kw):
    return jnp.dot(a, b, preferred_element_type=F32, **kw)


def rope_tables(pos_t, pos_h, pos_w):
    half_dim = HD // 2
    freq_index = jnp.arange(half_dim, dtype=jnp.int32)
    inverse = THETA ** (-(2.0 * freq_index.astype(F32)) / HD)
    first_cut = HD // 8
    second_cut = first_cut + 3 * HD // 16
    chosen = jnp.where(
        freq_index[None, :] < first_cut,
        pos_t[:, None],
        jnp.where(freq_index[None, :] < second_cut, pos_h[:, None], pos_w[:, None]),
    )
    angles = chosen.astype(F32) * inverse[None, :]
    return (jnp.cos(angles), jnp.sin(angles))


def rotate(vectors, cosine, sines):
    half_dim = vectors.shape[-1] // 2
    first_half = vectors[..., :half_dim]
    second_half = vectors[..., half_dim:]
    cos_part = cosine[:, None, :]
    sin_part = sines[:, None, :]
    return jnp.concatenate(
        [
            first_half * cos_part - second_half * sin_part,
            second_half * cos_part + first_half * sin_part,
        ],
        axis=-1,
    )


def shift(x, k):
    size = lax.axis_size("dp")
    return lax.ppermute(x, "dp", [(i, (i + k) % size) for i in range(size)])


def gather_dp(x):
    return [x] + [shift(x, k) for k in range(1, lax.axis_size("dp"))]


def gather_ctx(x):
    groups = lax.axis_size("ctx")
    own = lax.axis_index("ctx")
    if groups & (groups - 1):
        return lax.all_gather(x, "ctx", axis=0, tiled=True), jnp.arange(groups, dtype=jnp.int32)
    stride = groups // 2
    order = [0]
    while stride:
        other = lax.ppermute(x, "ctx", [(i, i ^ stride) for i in range(groups)])
        x = jnp.concatenate([x, other], axis=0)
        order = order + [b ^ stride for b in order]
        stride //= 2
    return x, own ^ jnp.asarray(order, jnp.int32)


def on_device(
    patches,
    vit_norm_gain,
    vit_qkv,
    vit_out,
    merger,
    text_embed,
    lang_norm_gain,
    key_weight,
    key_cotangent,
    image_grid,
    image_start,
):
    parts = lax.axis_size("dp")
    groups = lax.axis_size("ctx")
    own_part = lax.axis_index("dp")
    own = lax.axis_index("ctx")
    tokens, width = text_embed.shape[1:]
    vit_width = patches.shape[2]
    capacity = patches.shape[1] // 4
    attn_width = vit_qkv.shape[1] // 3
    key_width = key_weight.shape[1]
    head_count = attn_width // VHD // parts
    block_width = attn_width // parts
    feature_cols = merger.shape[1]

    info = jnp.concatenate([image_grid[0].T, image_start], axis=0)
    infos = jnp.stack(gather_dp(info))
    grid_rows, grid_cols, start_pos = infos[:, 0], infos[:, 1], infos[:, 2]
    counts = grid_rows * grid_cols
    target_range = start_pos // tokens
    group_index = jnp.arange(groups, dtype=jnp.int32)
    slot_index = jnp.arange(capacity, dtype=jnp.int32)
    own_counts = jnp.sum(jnp.where(group_index[None] == own, counts, 0), axis=1)

    row = jnp.arange(4 * capacity, dtype=jnp.int32)
    source_row = (row % capacity) * 4 + row // capacity
    order_rows = (source_row[:, None] == row[None, :]).astype(BF16)
    own_rows = dot(order_rows, patches[0]).astype(BF16)
    images = jnp.stack(gather_dp(own_rows))
    values = images.astype(F32)
    normed = (layer_norm(values) * vit_norm_gain).astype(BF16)
    part_width = vit_width // parts
    normed_part = lax.dynamic_slice_in_dim(normed, own_part * part_width, part_width, 2)
    qkv_blocks = vit_qkv.reshape(part_width, 3, parts, block_width)

    def head_weights(k):
        index = (own_part + k) % parts
        return lax.dynamic_index_in_dim(qkv_blocks, index, 2, keepdims=False).reshape(
            part_width, 3 * block_width
        )

    flat_part = normed_part.reshape(parts * 4 * capacity, part_width)
    projected = dot(flat_part, head_weights(0)).reshape(parts, 4 * capacity, -1)
    for k in range(1, parts):
        sent = dot(flat_part, head_weights(k)).astype(BF16).reshape(parts, 4 * capacity, -1)
        projected = projected + jnp.roll(shift(sent, k).astype(F32), k, axis=0)
    projected = projected.astype(BF16).reshape(parts, 4 * capacity, 3, head_count, VHD)
    scores = jnp.einsum(
        "iqhd,ikhd->ihqk", projected[:, :, 0], projected[:, :, 1], preferred_element_type=F32
    ) / math.sqrt(VHD)
    alive_mask = ((row % capacity)[None, :] < own_counts[:, None]).astype(F32)
    weights = jnp.exp(scores) * alive_mask[:, None, None, :]
    probability = (weights / jnp.sum(weights, axis=-1, keepdims=True)).astype(BF16)
    attended = jnp.einsum(
        "ihqk,ikhd->iqhd", probability, projected[:, :, 2], preferred_element_type=F32
    ).astype(BF16)
    out_part = dot(attended.reshape(parts * 4 * capacity, block_width), vit_out)
    out_part = out_part.reshape(parts, 4 * capacity, vit_width)

    places = max(1, 4 // parts)
    pieces = max(1, parts // 4)
    piece_width = vit_width // pieces

    def place_rows(array, index):
        return lax.dynamic_slice_in_dim(
            array, (index * 4 // parts) * capacity, places * capacity, 1
        )

    hidden_rows = place_rows(values, own_part) + place_rows(out_part, own_part)
    for k in range(1, parts):
        sent = place_rows(out_part, (own_part + k) % parts).astype(BF16)
        hidden_rows = hidden_rows + jnp.roll(shift(sent, k).astype(F32), k, axis=0)
    merged = layer_norm(hidden_rows).astype(BF16)
    keeping = slot_index[None, :] < own_counts[:, None]
    merged = jnp.where(
        keeping[:, None, :, None], merged.reshape(parts, places, capacity, vit_width), 0
    )
    merged = lax.dynamic_slice_in_dim(merged, (own_part % pieces) * piece_width, piece_width, 3)
    merged = jnp.swapaxes(merged, 1, 2).reshape(parts * capacity, places * piece_width)
    merged_all, owners = gather_ctx(merged)

    text = text_embed[0].astype(F32)
    text_scale = lax.rsqrt(jnp.mean(text * text, axis=-1, keepdims=True) + EPS)
    text_normed = (text * text_scale * lang_norm_gain).astype(BF16)
    part_features = width // parts

    def text_part(index):
        return lax.dynamic_slice_in_dim(text_normed, index * part_features, part_features, 1)

    text_rows = [text_part(own_part)]
    for k in range(1, parts):
        text_rows.append(shift(text_part((own_part + k) % parts), k))
    text_keys = dot(jnp.concatenate(text_rows, axis=0), key_weight).reshape(parts, tokens, -1)
    key_proj = text_keys[0]
    for k in range(1, parts):
        key_proj = key_proj + shift(text_keys[k].astype(BF16), -k).astype(F32)

    own_start = own * feature_cols
    holder_part = own_start // part_features
    candidate = lax.dynamic_slice_in_dim(key_weight, own_start % part_features, feature_cols, 0)
    key_rows = jnp.where(own_part == holder_part, candidate, jnp.zeros_like(candidate))
    held_by = [g * feature_cols // part_features for g in range(groups)]
    for k in range(1, parts):
        pairs = [
            (held_by[g] * groups + g, (held_by[g] + k) % parts * groups + g) for g in range(groups)
        ]
        key_rows = key_rows + lax.ppermute(candidate, ("dp", "ctx"), pairs)
    own_gain = lax.dynamic_slice_in_dim(lang_norm_gain, own_start, feature_cols, 0)

    own_range = target_range[0] == own
    image_first = jnp.sum(jnp.where(own_range, start_pos[0], 0))
    own_cols = jnp.sum(jnp.where(own_range, grid_cols[0], 0))
    image_count = jnp.sum(jnp.where(own_range, counts[0], 0))
    local_index = jnp.arange(tokens, dtype=jnp.int32)
    inner_index = local_index - (image_first - own * tokens)
    image_mask = (inner_index >= 0) & (inner_index < image_count)
    selector = (inner_index[:, None] == slot_index[None, :]) & (slot_index < image_count)[None, :]
    global_index = own * tokens + local_index
    inner_safe = jnp.clip(inner_index, 0, capacity - 1)
    pos_t = jnp.where(image_mask, image_first, global_index)
    pos_h = jnp.where(image_mask, image_first + inner_safe // own_cols, global_index)
    pos_w = jnp.where(image_mask, image_first + inner_safe % own_cols, global_index)
    cosine, sines = rope_tables(pos_t, pos_h, pos_w)
    grad_key = rotate(
        key_cotangent[0].astype(F32).reshape(tokens, key_width // HD, HD), cosine, -sines
    ).reshape(tokens, -1)
    grad_image_key = dot(selector.T.astype(F32), grad_key, precision=HIGHEST).astype(BF16)
    grads = jnp.concatenate(gather_dp(grad_image_key), axis=0)
    grads = lax.all_gather(grads, "ctx", axis=0, tiled=True)
    grads = grads.reshape(groups, parts, capacity, key_width)
    block_owner = (owners[:, None] == group_index[None, :]).astype(jnp.int32)
    block_range = jnp.sum(block_owner[None] * target_range[:, None, :], axis=-1)
    routing = (block_range[:, :, None] == group_index[None, None, :]).astype(BF16)
    grads = jnp.einsum("rih,hrkw->irkw", routing, grads, preferred_element_type=F32).astype(BF16)
    weighted = (
        lax.dot_general(
            grads.reshape(-1, key_width),
            key_rows,
            (((1,), (1,)), ((), ())),
            preferred_element_type=F32,
        )
        * own_gain
    )

    embed_part = dot(merged_all, merger).reshape(groups, parts, capacity, feature_cols)
    embedded = embed_part
    for k in range(1, parts):
        embedded = embedded + jnp.roll(shift(embed_part.astype(BF16), k).astype(F32), k, axis=1)
    embedded = embedded.reshape(-1, feature_cols).astype(BF16)
    values = embedded.astype(F32)
    sums = jnp.stack([jnp.sum(values * values, axis=-1), jnp.sum(values * weighted, axis=-1)])
    sums = jnp.swapaxes(sums.reshape(2, groups, -1), 0, 1).reshape(groups, -1)
    block_owner = block_owner.astype(F32)
    sums = dot(block_owner.T, sums, precision=HIGHEST)
    sums = lax.all_to_all(
        jnp.broadcast_to(sums[None], (groups,) + sums.shape), "ctx", 0, 0, tiled=True
    )
    sums = dot(block_owner, jnp.sum(sums, axis=0), precision=HIGHEST).reshape(groups, 2, -1)
    row_scale = lax.rsqrt(sums[:, 0] / width + EPS)
    slope = (row_scale**3 * sums[:, 1] / width).reshape(-1, 1)
    grad_embedded = (row_scale.reshape(-1, 1) * weighted - values * slope).astype(BF16)
    merger_grad = lax.dot_general(
        merged_all, grad_embedded, (((0,), (0,)), ((), ())), preferred_element_type=F32
    )

    own_seq = values.reshape(groups, parts, capacity, feature_cols)[:, 0] * own_gain
    image_part = dot(own_seq.reshape(-1, feature_cols).astype(BF16), key_rows).astype(BF16)
    outgoing = jnp.einsum(
        "ih,ikw->hkw",
        routing[0],
        image_part.reshape(groups, capacity, key_width),
        preferred_element_type=F32,
    ).astype(BF16)
    arrived = lax.all_to_all(outgoing, "ctx", 0, 0, tiled=True)
    image_scale = jnp.sum(
        jnp.where(
            (block_range[0] == own)[:, None],
            row_scale.reshape(groups, parts, capacity)[:, 0],
            0.0,
        ),
        axis=0,
    )
    image_keys = jnp.sum(arrived.astype(F32), axis=0) * image_scale[:, None]
    placed = dot(selector.astype(F32), image_keys, precision=HIGHEST)
    key_proj = jnp.where(image_mask[:, None], placed, key_proj)
    rotated = (
        rotate(key_proj.reshape(tokens, key_width // HD, HD), cosine, sines)
        .reshape(tokens, -1)
        .astype(BF16)
    )
    return (rotated[None], merger_grad)


def solution(mesh):
    return jax.shard_map(
        on_device,
        mesh=mesh,
        in_specs=(
            P("dp", "ctx", None),
            P(),
            P("dp", None),
            P("dp", None),
            P("dp", "ctx"),
            P("dp", "ctx", None),
            P(),
            P("dp", None),
            P("dp", "ctx", None),
            P("dp", None, None),
            P("dp", None),
        ),
        out_specs=(P("dp", "ctx", None), P("dp", "ctx")),
        check_vma=False,
    )
```

```python
import math

import jax
import jax.numpy as jnp
from jax import lax
from jax.experimental import pallas as pl
from jax.experimental.pallas import tpu as pltpu
from jax.sharding import PartitionSpec as P

VHD = 80
HD = 128
EPS = 1e-06
THETA = 1000000.0
HIGHEST = lax.Precision.HIGHEST
BF16 = jnp.bfloat16
F32 = jnp.float32


def layer_norm(values):
    average = jnp.mean(values, axis=-1, keepdims=True)
    centered = values - average
    variance = jnp.mean(centered * centered, axis=-1, keepdims=True)
    return centered * lax.rsqrt(variance + EPS)


def dot(a, b, **kw):
    return jnp.dot(a, b, preferred_element_type=F32, **kw)


def rope_tables(pos_t, pos_h, pos_w):
    half_dim = HD // 2
    freq_index = jnp.arange(half_dim, dtype=jnp.int32)
    inverse = THETA ** (-(2.0 * freq_index.astype(F32)) / HD)
    first_cut = HD // 8
    second_cut = first_cut + 3 * HD // 16
    chosen = jnp.where(
        freq_index[None, :] < first_cut,
        pos_t[:, None],
        jnp.where(freq_index[None, :] < second_cut, pos_h[:, None], pos_w[:, None]),
    )
    angles = chosen.astype(F32) * inverse[None, :]
    return (jnp.cos(angles), jnp.sin(angles))


def rotate(vectors, cosine, sines):
    half_dim = vectors.shape[-1] // 2
    first_half = vectors[..., :half_dim]
    second_half = vectors[..., half_dim:]
    cos_part = cosine[:, None, :]
    sin_part = sines[:, None, :]
    return jnp.concatenate(
        [
            first_half * cos_part - second_half * sin_part,
            second_half * cos_part + first_half * sin_part,
        ],
        axis=-1,
    )


def shift(x, k):
    size = lax.axis_size("dp")
    return lax.ppermute(x, "dp", [(i, (i + k) % size) for i in range(size)])


def gather_dp(x):
    return [x] + [shift(x, k) for k in range(1, lax.axis_size("dp"))]


def strides_of(size):
    return [1 << b for b in reversed(range(size.bit_length() - 1))]


def xor_gather(x, strides):
    size = lax.axis_size("ctx")
    pieces = [x]
    offsets = [[0]]
    for stride in strides:
        known = [o for piece in offsets for o in piece]
        joined = pieces[0] if len(pieces) == 1 else jnp.concatenate(pieces, axis=0)
        pieces.append(lax.ppermute(joined, "ctx", [(i, i ^ stride) for i in range(size)]))
        offsets.append([o ^ stride for o in known])
    return pieces, offsets


def gather_ctx(x):
    size = lax.axis_size("ctx")
    if size & (size - 1):
        return lax.all_gather(x, "ctx", axis=0, tiled=True), jnp.arange(size, dtype=jnp.int32)
    pieces, offsets = xor_gather(x, strides_of(size))
    order = [o for piece in offsets for o in piece]
    return jnp.concatenate(pieces, axis=0), lax.axis_index("ctx") ^ jnp.asarray(order, jnp.int32)


def gather_pieces(x):
    size = lax.axis_size("ctx")
    if size & (size - 1) or size < 8:
        x, owners = gather_ctx(x)
        return [(x, 0, list(range(size)))], owners
    strides = strides_of(size)
    middle = x.shape[1] // 2
    pieces, offsets = xor_gather(x[:, :middle], strides)
    order = [o for piece in offsets for o in piece]
    found = [(p, 0, [order.index(o) for o in piece]) for p, piece in zip(pieces, offsets)]
    pieces, offsets = xor_gather(x[:, middle:], strides[-2:-1] + strides[:-2] + strides[-1:])
    found += [(p, middle, [order.index(o) for o in piece]) for p, piece in zip(pieces, offsets)]
    return found, lax.axis_index("ctx") ^ jnp.asarray(order, jnp.int32)


SMEM = pl.BlockSpec(memory_space=pltpu.SMEM)
VMEM = pl.BlockSpec(memory_space=pltpu.VMEM)


def call(kernel, outs, ins, scalars=0, scratch=(), name=None):
    return pl.pallas_call(
        kernel,
        out_shape=outs,
        in_specs=[SMEM] * scalars + [VMEM] * (len(ins) - scalars),
        out_specs=[VMEM] * len(outs),
        scratch_shapes=list(scratch),
        name=name,
    )(*ins)


def project(parts, index, images, gain, weight):
    rows, width = images[0].shape
    depth, columns = weight.shape
    third = columns // 3
    block = third // parts

    def kernel(index_ref, *refs):
        image_refs = refs[:parts]
        gain_ref, weight_ref, mine_ref, sent_ref = refs[parts:]
        own = index_ref[0]
        pieces = []
        for r in range(parts):
            normed = layer_norm(image_refs[r][...].astype(F32)) * gain_ref[...]
            piece = normed[:, :depth]
            for b in range(1, parts):
                piece = jnp.where(own == b, normed[:, b * depth : (b + 1) * depth], piece)
            pieces.append(piece.astype(BF16))
        product = dot(jnp.concatenate(pieces, axis=0), weight_ref[...])
        for b in range(parts):
            heads = jnp.concatenate(
                [product[:, j * third + b * block : j * third + (b + 1) * block] for j in range(3)],
                axis=1,
            )

            @pl.when(own == b)
            def _():
                mine_ref[...] = heads.reshape(parts, rows, 3 * block)

            for k in range(1, parts):

                @pl.when((own + k) % parts == b)
                def _():
                    for r in range(parts):
                        sent_ref[k - 1, (r + k) % parts] = heads[r * rows : (r + 1) * rows].astype(
                            BF16
                        )

    return call(
        kernel,
        (
            jax.ShapeDtypeStruct((parts, rows, 3 * block), F32),
            jax.ShapeDtypeStruct((parts - 1, parts, rows, 3 * block), BF16),
        ),
        (index, *images, gain, weight),
        scalars=1,
        name="project",
    )


def attend(parts, places, scalars, mine, received, images, out_weight):
    rows, width = images[0].shape
    capacity = rows // 4
    block = out_weight.shape[0]
    heads = block // VHD
    taken = places * capacity

    def kernel(scalar_ref, *refs):
        mine_ref = refs[0]
        received_refs = refs[1:parts]
        image_refs = refs[parts : 2 * parts]
        weight_ref, hidden_ref, sent_ref, scratch = refs[2 * parts :]
        own = scalar_ref[0]
        lane = lax.broadcasted_iota(jnp.int32, (rows, block), 1)
        key_slot = lax.broadcasted_iota(jnp.int32, (heads * rows, rows), 1) % capacity
        attended = []
        for r in range(parts):
            total = mine_ref[r]
            for ref in received_refs:
                total = total + ref[r].astype(F32)
            total = total.astype(BF16)
            queries = total[:, :block]
            keys = total[:, block : 2 * block]
            contents = total[:, 2 * block :]
            in_head = [(lane >= h * VHD) & (lane < (h + 1) * VHD) for h in range(heads)]
            stacked = jnp.concatenate(
                [jnp.where(inside, queries, jnp.zeros_like(queries)) for inside in in_head], axis=0
            )
            scores = lax.dot_general(
                stacked, keys, (((1,), (1,)), ((), ())), preferred_element_type=F32
            ) / math.sqrt(VHD)
            alive = (key_slot < scalar_ref[1 + r]).astype(F32)
            weights = jnp.exp(scores) * alive
            probability = (weights / jnp.sum(weights, axis=-1, keepdims=True)).astype(BF16)
            spread = dot(probability, contents)
            picked = jnp.where(in_head[0], spread[:rows], 0.0)
            for h in range(1, heads):
                picked = picked + jnp.where(in_head[h], spread[h * rows : (h + 1) * rows], 0.0)
            attended.append(picked.astype(BF16))
        product = dot(jnp.concatenate(attended, axis=0), weight_ref[...])
        scratch[...] = product.reshape(parts, rows, width)

        def start(index):
            return pl.multiple_of((index * 4 // parts) * capacity, capacity)

        for r in range(parts):
            at = pl.ds(start(own), taken)
            hidden_ref[r] = scratch[r, at, :] + image_refs[r][at, :].astype(F32)
            for k in range(1, parts):
                at = pl.ds(start((own + k) % parts), taken)
                sent_ref[k - 1, (r + k) % parts] = scratch[r, at, :].astype(BF16)

    return call(
        kernel,
        (
            jax.ShapeDtypeStruct((parts, taken, width), F32),
            jax.ShapeDtypeStruct((parts - 1, parts, taken, width), BF16),
        ),
        (scalars, mine, *received, *images, out_weight),
        scalars=1,
        scratch=[pltpu.VMEM((parts, rows, width), F32)],
        name="attend",
    )


def embed(rows, groups, pieces, weight):
    depth, columns = weight.shape
    count = len(pieces)

    def kernel(*refs):
        weight_ref, merged_ref, part_ref, sent_ref = refs[count:]
        for ref, (array, column, blocks) in zip(refs[:count], pieces):
            for j, block in enumerate(blocks):
                merged_ref[block * rows : (block + 1) * rows, column : column + array.shape[1]] = ref[
                    j * rows : (j + 1) * rows
                ]
        product = dot(merged_ref[...], weight_ref[...])
        part_ref[...] = product
        sent_ref[...] = product.astype(BF16)

    total = groups * rows
    return call(
        kernel,
        (
            jax.ShapeDtypeStruct((total, depth), BF16),
            jax.ShapeDtypeStruct((total, columns), F32),
            jax.ShapeDtypeStruct((total, columns), BF16),
        ),
        (*[p[0] for p in pieces], weight),
        name="embed",
    )


def features(parts, groups, owners, holders, own_part, received, weighted, gain, key_rows):
    total, columns = own_part.shape
    rows = total // groups
    capacity = rows // parts
    key_width = key_rows.shape[1]
    count = len(received)

    def kernel(owner_ref, holder_ref, *refs):
        part_ref = refs[0]
        received_refs = refs[1 : 1 + count]
        weighted_ref, gain_ref, key_ref, embed_ref, sums_ref, keys_ref = refs[1 + count :]
        picked = []
        for i in range(groups):
            at = pl.ds(i * rows, rows)
            block = part_ref[at, :]
            for ref in received_refs:
                block = block + ref[at, :].astype(F32)
            block = block.astype(BF16)
            picked.append((block[:capacity].astype(F32) * gain_ref[...]).astype(BF16))
            embed_ref[pl.ds(pl.multiple_of(owner_ref[i] * rows, rows), rows), :] = block
        values = embed_ref[...].astype(F32)
        ones = jnp.ones((8, columns), F32)
        contract = (((1,), (1,)), ((), ()))
        squares = lax.dot_general(
            ones, values * values, contract, precision=HIGHEST, preferred_element_type=F32
        )
        products = lax.dot_general(
            ones, values * weighted_ref[...], contract, precision=HIGHEST, preferred_element_type=F32
        )
        for i in range(groups):
            sums_ref[i, 0:1] = squares[0:1]
            sums_ref[i, 1:2] = products[0:1]
        terms = dot(jnp.concatenate(picked, axis=0), key_ref[...]).astype(BF16)
        for i in range(groups):
            keys_ref[holder_ref[i]] = terms[i * capacity : (i + 1) * capacity]

    return call(
        kernel,
        (
            jax.ShapeDtypeStruct((total, columns), BF16),
            jax.ShapeDtypeStruct((groups, 2, total), F32),
            jax.ShapeDtypeStruct((groups, capacity, key_width), BF16),
        ),
        (owners, holders, own_part, *received, weighted, gain, key_rows),
        scalars=2,
        name="features",
    )


def finish(groups, width, owners, sums, embedded, weighted, merged):
    total, columns = embedded.shape
    rows = total // groups
    height = merged.shape[1]
    bands = 5 if height % (5 * 128) == 0 else 1
    band = height // bands

    def kernel(
        owner_ref, sums_ref, embed_ref, weighted_ref, merged_ref, out_ref, scale_ref, grads, ordered
    ):
        @pl.when(pl.program_id(0) == 0)
        def _():
            whole = jnp.sum(sums_ref[...], axis=0)
            scale = lax.rsqrt(whole[0:1] / width + EPS)
            slope = scale**3 * whole[1:2] / width
            line = lax.broadcasted_iota(jnp.int32, (8, total), 0)
            both = jnp.where(line == 0, scale, slope)
            scale_ref[...] = both
            columns_of = jnp.transpose(both)
            grads[...] = (
                columns_of[:, 0:1] * weighted_ref[...]
                - embed_ref[...].astype(F32) * columns_of[:, 1:2]
            ).astype(BF16)
            for i in range(groups):
                ordered[pl.ds(i * rows, rows), :] = grads[
                    pl.ds(pl.multiple_of(owner_ref[i] * rows, rows), rows), :
                ]

        out_ref[...] = lax.dot_general(
            merged_ref[...], ordered[...], (((0,), (0,)), ((), ())), preferred_element_type=F32
        )

    return pl.pallas_call(
        kernel,
        grid=(bands,),
        out_shape=(
            jax.ShapeDtypeStruct((height, columns), F32),
            jax.ShapeDtypeStruct((8, total), F32),
        ),
        in_specs=[
            SMEM,
            pl.BlockSpec(sums.shape, lambda g: (0, 0, 0)),
            pl.BlockSpec(embedded.shape, lambda g: (0, 0)),
            pl.BlockSpec(weighted.shape, lambda g: (0, 0)),
            pl.BlockSpec((total, band), lambda g: (0, g)),
        ],
        out_specs=[
            pl.BlockSpec((band, columns), lambda g: (g, 0)),
            pl.BlockSpec((8, total), lambda g: (0, 0)),
        ],
        scratch_shapes=[pltpu.VMEM((total, columns), BF16), pltpu.VMEM((total, columns), BF16)],
        compiler_params=pltpu.CompilerParams(dimension_semantics=("arbitrary",)),
        name="finish",
    )(owners, sums, embedded, weighted, merged)


def text_norm(parts, index, text, gain):
    tokens, width = text.shape
    step = 32 if tokens % 32 == 0 else tokens
    block = width // parts

    def kernel(index_ref, text_ref, gain_ref, out_ref, scratch):
        values = text_ref[...].astype(F32)
        scale = lax.rsqrt(jnp.mean(values * values, axis=-1, keepdims=True) + EPS)
        scratch[...] = (values * scale * gain_ref[...]).astype(BF16)
        for k in range(parts):
            start = pl.multiple_of((index_ref[0] + k) % parts * block, block)
            out_ref[k] = scratch[:, pl.ds(start, block)]

    return pl.pallas_call(
        kernel,
        grid=(tokens // step,),
        out_shape=jax.ShapeDtypeStruct((parts, tokens, block), BF16),
        in_specs=[
            SMEM,
            pl.BlockSpec((step, width), lambda g: (g, 0)),
            pl.BlockSpec((1, width), lambda g: (0, 0)),
        ],
        out_specs=pl.BlockSpec((parts, step, block), lambda g: (0, g, 0)),
        scratch_shapes=[pltpu.VMEM((step, width), BF16)],
        name="text_norm",
    )(index, text, gain)


def on_device(
    patches,
    vit_norm_gain,
    vit_qkv,
    vit_out,
    merger,
    text_embed,
    lang_norm_gain,
    key_weight,
    key_cotangent,
    image_grid,
    image_start,
):
    parts = lax.axis_size("dp")
    groups = lax.axis_size("ctx")
    own_part = lax.axis_index("dp")
    own = lax.axis_index("ctx")
    tokens, width = text_embed.shape[1:]
    vit_width = patches.shape[2]
    capacity = patches.shape[1] // 4
    key_width = key_weight.shape[1]
    feature_cols = merger.shape[1]

    info = jnp.concatenate([image_grid[0].T, image_start], axis=0)
    infos = jnp.stack(gather_dp(info))
    grid_rows, grid_cols, start_pos = infos[:, 0], infos[:, 1], infos[:, 2]
    counts = grid_rows * grid_cols
    target_range = start_pos // tokens
    group_index = jnp.arange(groups, dtype=jnp.int32)
    slot_index = jnp.arange(capacity, dtype=jnp.int32)
    own_counts = jnp.sum(jnp.where(group_index[None] == own, counts, 0), axis=1)

    row = jnp.arange(4 * capacity, dtype=jnp.int32)
    source_row = (row % capacity) * 4 + row // capacity
    order_rows = (source_row[:, None] == row[None, :]).astype(BF16)
    own_rows = dot(order_rows, patches[0]).astype(BF16)
    images = gather_dp(own_rows)
    part_index = own_part.astype(jnp.int32).reshape(1)
    mine, sent = project(parts, part_index, images, vit_norm_gain.reshape(1, -1), vit_qkv)
    received = [shift(sent[k - 1], k) for k in range(1, parts)]
    places = max(1, 4 // parts)
    pieces = max(1, parts // 4)
    piece_width = vit_width // pieces
    scalars = jnp.concatenate([part_index, own_counts])
    hidden_rows, sent = attend(parts, places, scalars, mine, received, images, vit_out)
    for k in range(1, parts):
        hidden_rows = hidden_rows + shift(sent[k - 1], k).astype(F32)
    merged = layer_norm(hidden_rows).astype(BF16)
    keeping = slot_index[None, :] < own_counts[:, None]
    merged = jnp.where(
        keeping[:, None, :, None], merged.reshape(parts, places, capacity, vit_width), 0
    )
    merged = lax.dynamic_slice_in_dim(merged, (own_part % pieces) * piece_width, piece_width, 3)
    merged = jnp.swapaxes(merged, 1, 2).reshape(parts * capacity, places * piece_width)
    merged_pieces, owners = gather_pieces(merged)

    gain_line = lang_norm_gain.reshape(1, -1)
    text_blocks = text_norm(parts, part_index, text_embed[0], gain_line)
    part_features = width // parts
    text_rows = [text_blocks[0]] + [shift(text_blocks[k], k) for k in range(1, parts)]
    text_keys = dot(jnp.concatenate(text_rows, axis=0), key_weight).reshape(parts, tokens, -1)
    key_proj = text_keys[0]
    for k in range(1, parts):
        key_proj = key_proj + shift(text_keys[k].astype(BF16), -k).astype(F32)

    own_start = own * feature_cols
    holder_part = own_start // part_features
    candidate = lax.dynamic_slice_in_dim(key_weight, own_start % part_features, feature_cols, 0)
    key_rows = jnp.where(own_part == holder_part, candidate, jnp.zeros_like(candidate))
    held_by = [g * feature_cols // part_features for g in range(groups)]
    for k in range(1, parts):
        pairs = [
            (held_by[g] * groups + g, (held_by[g] + k) % parts * groups + g) for g in range(groups)
        ]
        key_rows = key_rows + lax.ppermute(candidate, ("dp", "ctx"), pairs)
    own_gain = lax.dynamic_slice_in_dim(lang_norm_gain, own_start, feature_cols, 0).reshape(1, -1)

    own_range = target_range[0] == own
    image_first = jnp.sum(jnp.where(own_range, start_pos[0], 0))
    own_cols = jnp.sum(jnp.where(own_range, grid_cols[0], 0))
    image_count = jnp.sum(jnp.where(own_range, counts[0], 0))
    local_index = jnp.arange(tokens, dtype=jnp.int32)
    inner_index = local_index - (image_first - own * tokens)
    image_mask = (inner_index >= 0) & (inner_index < image_count)
    selector = (inner_index[:, None] == slot_index[None, :]) & (slot_index < image_count)[None, :]
    global_index = own * tokens + local_index
    inner_safe = jnp.clip(inner_index, 0, capacity - 1)
    pos_t = jnp.where(image_mask, image_first, global_index)
    pos_h = jnp.where(image_mask, image_first + inner_safe // own_cols, global_index)
    pos_w = jnp.where(image_mask, image_first + inner_safe % own_cols, global_index)
    cosine, sines = rope_tables(pos_t, pos_h, pos_w)
    grad_key = rotate(
        key_cotangent[0].astype(F32).reshape(tokens, key_width // HD, HD), cosine, -sines
    ).reshape(tokens, -1)
    grad_image_key = dot(selector.T.astype(F32), grad_key, precision=HIGHEST).astype(BF16)
    grads = jnp.concatenate(gather_dp(grad_image_key), axis=0)
    grads, _ = gather_ctx(grads)
    grads = grads.reshape(groups, parts, capacity, key_width)
    routing = (target_range[:, :, None] == owners[None, None, :]).astype(BF16)
    grads = jnp.einsum("roi,irkw->orkw", routing, grads, preferred_element_type=F32).astype(BF16)
    weighted = (
        lax.dot_general(
            grads.reshape(-1, key_width),
            key_rows,
            (((1,), (1,)), ((), ())),
            preferred_element_type=F32,
        )
        * own_gain
    )

    merged_all, embed_part, embed_sent = embed(parts * capacity, groups, merged_pieces, merger)
    embed_sent = embed_sent.reshape(groups, parts, capacity, feature_cols)
    received = [
        jnp.roll(shift(embed_sent, k), k, axis=1).reshape(-1, feature_cols)
        for k in range(1, parts)
    ]
    block_owner = (owners[:, None] == group_index[None, :]).astype(jnp.int32)
    block_range = jnp.sum(block_owner * target_range[0][None, :], axis=-1)
    embedded, sums, outgoing = features(
        parts, groups, owners, block_range, embed_part, received, weighted, own_gain, key_rows
    )
    sums = lax.all_to_all(sums, "ctx", 0, 0, tiled=True)
    arrived = lax.all_to_all(outgoing, "ctx", 0, 0, tiled=True)
    merger_grad, scales = finish(
        groups, float(width), owners, sums, embedded, weighted, merged_all
    )

    image_scale = jnp.sum(
        jnp.where(
            (target_range[0] == own)[:, None],
            scales[0].reshape(groups, parts, capacity)[:, 0],
            0.0,
        ),
        axis=0,
    )
    image_keys = jnp.sum(arrived.astype(F32), axis=0) * image_scale[:, None]
    placed = dot(selector.astype(F32), image_keys, precision=HIGHEST)
    key_proj = jnp.where(image_mask[:, None], placed, key_proj)
    rotated = (
        rotate(key_proj.reshape(tokens, key_width // HD, HD), cosine, sines)
        .reshape(tokens, -1)
        .astype(BF16)
    )
    return (rotated[None], merger_grad)


def solution(mesh):
    return jax.shard_map(
        on_device,
        mesh=mesh,
        in_specs=(
            P("dp", "ctx", None),
            P(),
            P("dp", None),
            P("dp", None),
            P("dp", "ctx"),
            P("dp", "ctx", None),
            P(),
            P("dp", None),
            P("dp", "ctx", None),
            P("dp", None, None),
            P("dp", None),
        ),
        out_specs=(P("dp", "ctx", None), P("dp", "ctx")),
        check_vma=False,
    )
```

```python
import math

import jax
import jax.numpy as jnp
from jax import lax
from jax.experimental import pallas as pl
from jax.experimental.pallas import tpu as pltpu
from jax.sharding import PartitionSpec as P


VHD = 80
HD = 128
EPS = 1e-06
THETA = 1000000.0
HIGHEST = lax.Precision.HIGHEST
BF16 = jnp.bfloat16
barrier = lax.optimization_barrier
F32 = jnp.float32


def layer_norm(values):
    average = jnp.mean(values, axis=-1, keepdims=True)
    centered = values - average
    variance = jnp.mean(centered * centered, axis=-1, keepdims=True)
    return centered * lax.rsqrt(variance + EPS)


def dot(a, b, **kw):
    return jnp.dot(a, b, preferred_element_type=F32, **kw)


def shift(x, k):
    size = lax.axis_size("dp")
    return lax.ppermute(x, "dp", [(i, (i + k) % size) for i in range(size)])


def gather_dp(x):
    return [x] + [shift(x, k) for k in range(1, lax.axis_size("dp"))]


def strides_of(size):
    return [1 << b for b in reversed(range(size.bit_length() - 1))]


def xor_gather(x, strides):
    size = lax.axis_size("ctx")
    pieces = [x]
    offsets = [[0]]
    for stride in strides:
        known = [o for piece in offsets for o in piece]
        joined = pieces[0] if len(pieces) == 1 else jnp.concatenate(pieces, axis=0)
        pieces.append(lax.ppermute(joined, "ctx", [(i, i ^ stride) for i in range(size)]))
        offsets.append([o ^ stride for o in known])
    return pieces, offsets


def gather_halves(x):
    size = lax.axis_size("ctx")
    own = lax.axis_index("ctx")
    if size & (size - 1) or size < 8:
        return [lax.all_gather(x, "ctx", axis=0, tiled=True)], jnp.arange(size, dtype=jnp.int32)
    strides = strides_of(size)
    middle = x.shape[1] // 2
    left, offsets = xor_gather(x[:, :middle], strides[:-1])
    right, others = xor_gather(x[:, middle:], strides[-2:-1] + strides[:-2])
    order = [o for piece in offsets for o in piece]
    rows = x.shape[0]
    found = {
        o: piece[j * rows : (j + 1) * rows]
        for piece, known in zip(right, others)
        for j, o in enumerate(known)
    }
    low = jnp.concatenate(
        [jnp.concatenate(left, axis=0), jnp.concatenate([found[o] for o in order], axis=0)], axis=1
    )
    high = lax.ppermute(low, "ctx", [(i, i ^ 1) for i in range(size)])
    order = order + [o ^ 1 for o in order]
    return [low, high], own ^ jnp.asarray(order, jnp.int32)


def find_image(own, tokens, grid_ref, start_ref, groups):
    zero = jnp.int32(0)
    first, cols, count, owner = zero, zero, zero, zero
    for o in range(groups):
        start = start_ref[0, o]
        here = (start >= own * tokens) & (start < (own + 1) * tokens)
        first = jnp.where(here, start, first)
        cols = jnp.where(here, grid_ref[0, o, 1], cols)
        count = jnp.where(here, grid_ref[0, o, 0] * grid_ref[0, o, 1], count)
        owner = jnp.where(here, o, owner)
    return first, cols, count, owner


SMEM = pl.BlockSpec(memory_space=pltpu.SMEM)
VMEM = pl.BlockSpec(memory_space=pltpu.VMEM)


def call(kernel, outs, ins, scalars=0, scratch=()):
    return pl.pallas_call(
        kernel,
        out_shape=outs,
        in_specs=[SMEM] * scalars + [VMEM] * (len(ins) - scalars),
        out_specs=[VMEM] * len(outs),
        scratch_shapes=list(scratch),
    )(*ins)


def project(parts, index, images, gain, weight):
    rows, _ = images[0].shape
    depth, columns = weight.shape
    third = columns // 3
    block = third // parts

    def kernel(index_ref, *refs):
        image_refs = refs[:parts]
        gain_ref, weight_ref, mine_ref, sent_ref = refs[parts:]
        own = index_ref[0]
        pieces = []
        for r in range(parts):
            normed = layer_norm(image_refs[r][...].astype(F32)) * gain_ref[...]
            piece = normed[:, :depth]
            for b in range(1, parts):
                piece = jnp.where(own == b, normed[:, b * depth : (b + 1) * depth], piece)
            pieces.append(piece.astype(BF16))
        product = dot(jnp.concatenate(pieces, axis=0), weight_ref[...])
        for b in range(parts):
            heads = jnp.concatenate(
                [product[:, j * third + b * block : j * third + (b + 1) * block] for j in range(3)],
                axis=1,
            )

            @pl.when(own == b)
            def _():
                mine_ref[...] = heads.reshape(parts, rows, 3 * block)

            for k in range(1, parts):

                @pl.when((own + k) % parts == b)
                def _():
                    for r in range(parts):
                        sent_ref[k - 1, (r + k) % parts] = heads[r * rows : (r + 1) * rows].astype(
                            BF16
                        )

    return call(
        kernel,
        (
            jax.ShapeDtypeStruct((parts, rows, 3 * block), F32),
            jax.ShapeDtypeStruct((parts - 1, parts, rows, 3 * block), BF16),
        ),
        (index, *images, gain, weight),
        scalars=1,
    )


def attend(parts, places, scalars, mine, received, images, out_weight):
    rows, width = images[0].shape
    capacity = rows // 4
    block = out_weight.shape[0]
    heads = block // VHD
    taken = places * capacity

    def kernel(scalar_ref, *refs):
        mine_ref = refs[0]
        received_refs = refs[1:parts]
        image_refs = refs[parts : 2 * parts]
        weight_ref, hidden_ref, sent_ref, scratch = refs[2 * parts :]
        own = scalar_ref[0]
        lane = lax.broadcasted_iota(jnp.int32, (rows, block), 1)
        key_slot = lax.broadcasted_iota(jnp.int32, (heads * rows, rows), 1) % capacity
        attended = []
        for r in range(parts):
            total = mine_ref[r]
            for ref in received_refs:
                total = total + ref[r].astype(F32)
            total = total.astype(BF16)
            queries = total[:, :block]
            keys = total[:, block : 2 * block]
            contents = total[:, 2 * block :]
            in_head = [(lane >= h * VHD) & (lane < (h + 1) * VHD) for h in range(heads)]
            stacked = jnp.concatenate(
                [jnp.where(inside, queries, jnp.zeros_like(queries)) for inside in in_head], axis=0
            )
            scores = lax.dot_general(
                stacked, keys, (((1,), (1,)), ((), ())), preferred_element_type=F32
            ) / math.sqrt(VHD)
            alive = (key_slot < scalar_ref[1 + r]).astype(F32)
            weights = jnp.exp(scores) * alive
            probability = (weights / jnp.sum(weights, axis=-1, keepdims=True)).astype(BF16)
            spread = dot(probability, contents)
            picked = jnp.where(in_head[0], spread[:rows], 0.0)
            for h in range(1, heads):
                picked = picked + jnp.where(in_head[h], spread[h * rows : (h + 1) * rows], 0.0)
            attended.append(picked.astype(BF16))
        product = dot(jnp.concatenate(attended, axis=0), weight_ref[...])
        scratch[...] = product.reshape(parts, rows, width)

        def start(index):
            return pl.multiple_of((index * 4 // parts) * capacity, capacity)

        for r in range(parts):
            at = pl.ds(start(own), taken)
            hidden_ref[r] = scratch[r, at, :] + image_refs[r][at, :].astype(F32)
            for k in range(1, parts):
                at = pl.ds(start((own + k) % parts), taken)
                sent_ref[k - 1, (r + k) % parts] = scratch[r, at, :].astype(BF16)

    return call(
        kernel,
        (
            jax.ShapeDtypeStruct((parts, taken, width), F32),
            jax.ShapeDtypeStruct((parts - 1, parts, taken, width), BF16),
        ),
        (scalars, mine, *received, *images, out_weight),
        scalars=1,
        scratch=[pltpu.VMEM((parts, rows, width), F32)],
    )


def features(parts, groups, owners, holders, own_parts, received, weighted, gain, key_rows):
    total = sum(p.shape[0] for p in own_parts)
    columns = own_parts[0].shape[1]
    rows = total // groups
    capacity = rows // parts
    key_width = key_rows.shape[1]
    chunks = len(own_parts)
    per_chunk = groups // chunks
    flat = [r for group in received for r in group]

    def kernel(owner_ref, holder_ref, *refs):
        part_refs = refs[:chunks]
        received_refs = refs[chunks : chunks + len(flat)]
        weighted_ref, gain_ref, key_ref, embed_ref, sums_ref, keys_ref = refs[chunks + len(flat) :]
        picked = []
        for i in range(groups):
            chunk, base = i // per_chunk, (i % per_chunk) * rows
            block = part_refs[chunk][base : base + rows, :]
            for k in range(1, parts):
                ref = received_refs[chunk * (parts - 1) + k - 1]
                block = block + jnp.concatenate(
                    [
                        ref[pl.ds(base + (r - k) % parts * capacity, capacity), :].astype(F32)
                        for r in range(parts)
                    ],
                    axis=0,
                )
            block = block.astype(BF16)
            picked.append((block[:capacity].astype(F32) * gain_ref[...]).astype(BF16))
            embed_ref[pl.ds(pl.multiple_of(owner_ref[i] * rows, rows), rows), :] = block
        values = embed_ref[...].astype(F32)
        ones = jnp.ones((8, columns), F32)
        contract = (((1,), (1,)), ((), ()))
        squares = lax.dot_general(
            ones, values * values, contract, precision=HIGHEST, preferred_element_type=F32
        )
        products = lax.dot_general(
            ones, values * weighted_ref[...], contract, precision=HIGHEST, preferred_element_type=F32
        )
        for i in range(groups):
            sums_ref[i, :, 0:total] = squares[0:1]
            sums_ref[i, :, total : 2 * total] = products[0:1]
        terms = dot(jnp.concatenate(picked, axis=0), key_ref[...]).astype(BF16)
        for i in range(groups):
            keys_ref[holder_ref[i]] = terms[i * capacity : (i + 1) * capacity]

    return call(
        kernel,
        (
            jax.ShapeDtypeStruct((total, columns), BF16),
            jax.ShapeDtypeStruct((groups, 1, 2 * total), F32),
            jax.ShapeDtypeStruct((groups, capacity, key_width), BF16),
        ),
        (owners, holders, *own_parts, *flat, weighted, gain, key_rows),
        scalars=2,
    )


def finish(groups, width, owners, sums, embedded, weighted, merged):
    total, columns = embedded.shape
    rows = total // groups
    chunks = len(merged)
    chunk = total // chunks
    height = merged[0].shape[1]
    bands = 5 if height % (5 * 128) == 0 else 1
    band = height // bands

    def kernel(owner_ref, sums_ref, embed_ref, weighted_ref, *refs):
        merged_refs = refs[:chunks]
        out_ref, scale_ref, grads, ordered = refs[chunks:]

        @pl.when(pl.program_id(0) == 0)
        def _():
            whole = jnp.sum(sums_ref[...], axis=0)
            scale = lax.rsqrt(whole[:, :total] / width + EPS)
            slope = scale**3 * whole[:, total:] / width
            line = lax.broadcasted_iota(jnp.int32, (8, total), 0)
            both = jnp.where(line == 0, scale, slope)
            scale_ref[...] = both
            columns_of = jnp.transpose(both)
            grads[...] = (
                columns_of[:, 0:1] * weighted_ref[...]
                - embed_ref[...].astype(F32) * columns_of[:, 1:2]
            ).astype(BF16)
            for i in range(groups):
                ordered[pl.ds(i * rows, rows), :] = grads[
                    pl.ds(pl.multiple_of(owner_ref[i] * rows, rows), rows), :
                ]

        result = None
        for j in range(chunks):
            term = lax.dot_general(
                merged_refs[j][...],
                ordered[j * chunk : (j + 1) * chunk, :],
                (((0,), (0,)), ((), ())),
                preferred_element_type=F32,
            )
            result = term if result is None else result + term
        out_ref[...] = result

    return pl.pallas_call(
        kernel,
        grid=(bands,),
        out_shape=(
            jax.ShapeDtypeStruct((height, columns), F32),
            jax.ShapeDtypeStruct((8, total), F32),
        ),
        in_specs=[
            SMEM,
            pl.BlockSpec(sums.shape, lambda g: (0, 0, 0)),
            pl.BlockSpec(embedded.shape, lambda g: (0, 0)),
            pl.BlockSpec(weighted.shape, lambda g: (0, 0)),
        ]
        + [pl.BlockSpec((chunk, band), lambda g: (0, g))] * chunks,
        out_specs=[
            pl.BlockSpec((band, columns), lambda g: (g, 0)),
            pl.BlockSpec((8, total), lambda g: (0, 0)),
        ],
        scratch_shapes=[pltpu.VMEM((total, columns), BF16), pltpu.VMEM((total, columns), BF16)],
        compiler_params=pltpu.CompilerParams(dimension_semantics=("arbitrary",)),
        name="finish",
    )(owners, sums, embedded, weighted, *merged)


def merge(parts, places, counts, hidden, received):
    taken, width = hidden.shape[1:]
    capacity = taken // places

    def kernel(count_ref, *refs):
        hidden_ref, received_refs, out_ref = refs[0], refs[1:-1], refs[-1]
        slot = lax.broadcasted_iota(jnp.int32, (capacity, width), 0)
        for r in range(parts):
            total = hidden_ref[r]
            for ref in received_refs:
                total = total + ref[r].astype(F32)
            normed = layer_norm(total).astype(BF16)
            for p in range(places):
                kept = normed[p * capacity : (p + 1) * capacity]
                kept = jnp.where(slot < count_ref[r], kept, jnp.zeros_like(kept))
                out_ref[r * capacity : (r + 1) * capacity, p * width : (p + 1) * width] = kept

    return call(
        kernel,
        (jax.ShapeDtypeStruct((parts * capacity, places * width), BF16),),
        (counts, hidden, *received),
        scalars=1,
    )[0]


def angle_table(tokens, groups, capacity, index, grid, start):
    half = HD // 2
    first_cut = HD // 8
    second_cut = first_cut + 3 * HD // 16
    inverse = THETA ** (-(2.0 * (jnp.arange(HD, dtype=jnp.int32) % half).astype(F32)) / HD)

    def kernel(index_ref, grid_ref, start_ref, inverse_ref, out_ref):
        own = index_ref[1]
        first, cols, count, _ = find_image(own, tokens, grid_ref, start_ref, groups)
        line = lax.broadcasted_iota(jnp.int32, (tokens, HD), 0) + own * tokens
        frequency = lax.broadcasted_iota(jnp.int32, (tokens, HD), 1) % half
        inner = line - first
        row = jnp.zeros_like(inner)
        for j in range(1, capacity):
            row = row + (inner >= j * cols).astype(jnp.int32)
        offset = jnp.where(frequency < second_cut, row, inner - row * cols)
        offset = jnp.where(frequency < first_cut, 0, offset)
        inside = (inner >= 0) & (inner < count)
        chosen = jnp.where(inside, first + offset, line)
        out_ref[...] = chosen.astype(F32) * inverse_ref[...]

    return call(
        kernel,
        (jax.ShapeDtypeStruct((tokens, HD), F32),),
        (index, grid, start, inverse.reshape(1, -1)),
        scalars=3,
    )[0]


def place_rows(tokens, own, first, count, shape, axis):
    token = lax.broadcasted_iota(jnp.int32, shape, axis)
    slot = lax.broadcasted_iota(jnp.int32, shape, 1 - axis)
    return ((token + own * tokens - first == slot) & (slot < count)).astype(F32)


def turn(values, cosine, sines):
    heads = []
    for h in range(values.shape[1] // HD):
        head = values[:, h * HD : (h + 1) * HD]
        heads.append(head * cosine + pltpu.roll(head, HD // 2, 1) * sines)
    return jnp.concatenate(heads, axis=1)


def image_grads(tokens, groups, capacity, index, grid, start, cotangent, cosine, sines):
    width = cotangent.shape[1]

    def kernel(index_ref, grid_ref, start_ref, cotangent_ref, cosine_ref, sine_ref, out_ref):
        own = index_ref[1]
        first, _, count, _ = find_image(own, tokens, grid_ref, start_ref, groups)
        lane = lax.broadcasted_iota(jnp.int32, (tokens, HD), 1)
        signed = jnp.where(lane < HD // 2, sine_ref[...], -sine_ref[...])
        grad = turn(cotangent_ref[...].astype(F32), cosine_ref[...], signed)
        chosen = place_rows(tokens, own, first, count, (capacity, tokens), 1)
        out_ref[...] = dot(chosen, grad, precision=HIGHEST).astype(BF16)

    return call(
        kernel,
        (jax.ShapeDtypeStruct((capacity, width), BF16),),
        (index, grid, start, cotangent, cosine, sines),
        scalars=3,
    )[0]


def keys_out(parts, groups, index, grid, start, text_keys, returned, arrived, scales, cosine, sines):
    tokens, width = returned[0][0].shape[0] * len(returned), text_keys[0].shape[1]
    capacity = arrived.shape[1]
    total = scales.shape[1]
    chunks = len(text_keys)
    chunk = tokens // chunks
    flat = [r for group in returned for r in group]

    def kernel(index_ref, grid_ref, start_ref, *refs):
        text_refs = refs[:chunks]
        returned_refs = refs[chunks : chunks + len(flat)]
        arrived_ref, scale_ref, cosine_ref, sine_ref, out_ref = refs[chunks + len(flat) :]
        own = index_ref[1]
        first, _, count, owner = find_image(own, tokens, grid_ref, start_ref, groups)
        shape = (capacity, total)
        lane = lax.broadcasted_iota(jnp.int32, shape, 1)
        slot = lax.broadcasted_iota(jnp.int32, shape, 0)
        wanted = lane == owner * (parts * capacity) + slot
        scale = jnp.sum(jnp.where(wanted, scale_ref[0:1, :], 0.0), axis=-1, keepdims=True)
        image = jnp.sum(arrived_ref[...].astype(F32), axis=0) * scale
        chosen = place_rows(tokens, own, first, count, (tokens, capacity), 0)
        placed = dot(chosen, image, precision=HIGHEST)
        token = lax.broadcasted_iota(jnp.int32, (tokens, width), 0) + own * tokens
        inside = (token >= first) & (token < first + count)
        lane = lax.broadcasted_iota(jnp.int32, (tokens, HD), 1)
        signed = jnp.where(lane < HD // 2, -sine_ref[...], sine_ref[...])
        rows = []
        for j in range(chunks):
            part = text_refs[j][0:chunk, :]
            for k in range(parts - 1):
                part = part + returned_refs[j * (parts - 1) + k][...].astype(F32)
            rows.append(part)
        keys = jnp.where(inside, placed, jnp.concatenate(rows, axis=0))
        out_ref[...] = turn(keys, cosine_ref[...], signed).astype(BF16)

    return call(
        kernel,
        (jax.ShapeDtypeStruct((tokens, width), BF16),),
        (index, grid, start, *text_keys, *flat, arrived, scales, cosine, sines),
        scalars=3,
    )[0]


def text_norm(parts, chunks, index, text, gain):
    tokens, width = text.shape
    step = 32 if tokens // chunks % 32 == 0 else tokens // chunks
    block = width // parts
    steps = tokens // chunks // step

    def kernel(index_ref, text_ref, gain_ref, *refs):
        out_refs, scratch = refs[:-1], refs[-1]
        values = text_ref[...].astype(F32)
        scale = lax.rsqrt(jnp.mean(values * values, axis=-1, keepdims=True) + EPS)
        scratch[...] = (values * scale * gain_ref[...]).astype(BF16)
        for j in range(chunks):

            @pl.when(pl.program_id(0) // steps == j)
            def _():
                for k in range(parts):
                    start = pl.multiple_of((index_ref[0] + k) % parts * block, block)
                    out_refs[j * parts + k][...] = scratch[:, pl.ds(start, block)]

    def place(j):
        return lambda g: (jnp.clip(g - j * steps, 0, steps - 1), 0)

    flat = pl.pallas_call(
        kernel,
        grid=(tokens // step,),
        out_shape=[jax.ShapeDtypeStruct((tokens // chunks, block), BF16)] * (chunks * parts),
        in_specs=[
            SMEM,
            pl.BlockSpec((step, width), lambda g: (g, 0)),
            pl.BlockSpec((1, width), lambda g: (0, 0)),
        ],
        out_specs=[
            pl.BlockSpec((step, block), place(j)) for j in range(chunks) for _ in range(parts)
        ],
        scratch_shapes=[pltpu.VMEM((step, width), BF16)],
        name="text_norm",
    )(index, text, gain)
    return [flat[j * parts : (j + 1) * parts] for j in range(chunks)]


def on_device(
    patches,
    vit_norm_gain,
    vit_qkv,
    vit_out,
    merger,
    text_embed,
    lang_norm_gain,
    key_weight,
    key_cotangent,
    image_grid,
    image_start,
):
    parts = lax.axis_size("dp")
    groups = lax.axis_size("ctx")
    own_part = lax.axis_index("dp")
    own = lax.axis_index("ctx")
    tokens, width = text_embed.shape[1:]
    vit_width = patches.shape[2]
    capacity = patches.shape[1] // 4
    key_width = key_weight.shape[1]
    feature_cols = merger.shape[1]
    gain_line = lang_norm_gain.reshape(1, -1)
    index = jnp.stack([own_part, own]).astype(jnp.int32)
    others = range(1, parts)

    row = jnp.arange(4 * capacity, dtype=jnp.int32)
    source_row = (row % capacity) * 4 + row // capacity
    order_rows = (source_row[:, None] == row[None, :]).astype(BF16)
    images = gather_dp(dot(order_rows, patches[0]).astype(BF16))

    info = jnp.concatenate([image_grid[0].T, image_start], axis=0)
    infos = jnp.stack(gather_dp(info))
    counts = infos[:, 0] * infos[:, 1]
    target_range = infos[:, 2] // tokens
    group_index = jnp.arange(groups, dtype=jnp.int32)
    own_counts = jnp.sum(jnp.where(group_index[None] == own, counts, 0), axis=1)

    chunks = 2
    text_blocks = text_norm(parts, chunks, index, text_embed[0], gain_line)

    mine, sent = project(parts, index, images, vit_norm_gain.reshape(1, -1), vit_qkv)

    sent, grid, start = barrier((sent, image_grid, image_start))
    received = [shift(sent[k - 1], k) for k in others]
    angles = angle_table(tokens, groups, capacity, index, grid, start)
    cosine, sines = jnp.cos(angles), jnp.sin(angles)
    grads = image_grads(
        tokens, groups, capacity, index, grid, start, key_cotangent[0], cosine, sines
    )
    grads = jnp.concatenate(gather_dp(grads), axis=0)

    places = max(1, 4 // parts)
    pieces = max(1, parts // 4)
    piece_width = vit_width // pieces
    scalars = jnp.concatenate([index[:1], own_counts])
    hidden_rows, sent = attend(parts, places, scalars, mine, received, images, vit_out)
    sent, grads = barrier((sent, grads))
    received = [shift(sent[k - 1], k) for k in others]
    grads = lax.all_to_all(
        jnp.broadcast_to(grads[None], (groups,) + grads.shape), "ctx", 0, 0, tiled=True
    )
    received, text_blocks, key_source = barrier((received, text_blocks, key_weight))
    merged = merge(parts, places, own_counts, hidden_rows, received)
    if pieces > 1:
        merged = lax.dynamic_slice_in_dim(merged, (own_part % pieces) * piece_width, piece_width, 1)
    merged_all, owners = gather_halves(merged)

    part_features = width // parts
    own_start = own * feature_cols
    holder_part = own_start // part_features
    candidate = lax.dynamic_slice_in_dim(key_source, own_start % part_features, feature_cols, 0)
    key_rows = jnp.where(own_part == holder_part, candidate, jnp.zeros_like(candidate))
    held_by = [g * feature_cols // part_features for g in range(groups)]
    for k in others:
        pairs = [
            (held_by[g] * groups + g, (held_by[g] + k) % parts * groups + g) for g in range(groups)
        ]
        key_rows = key_rows + lax.ppermute(candidate, ("dp", "ctx"), pairs)
    own_gain = lax.dynamic_slice_in_dim(lang_norm_gain, own_start, feature_cols, 0).reshape(1, -1)

    def text_terms(blocks):
        rows = [blocks[0]] + [shift(blocks[k], k) for k in others]
        return dot(jnp.concatenate(rows, axis=0), key_weight)

    def text_return(terms):
        size = terms.shape[0] // parts
        return [shift(terms[k * size : (k + 1) * size].astype(BF16), -k) for k in others]

    early_terms = text_terms(text_blocks[0])

    grads = grads.reshape(groups, parts, capacity, key_width)
    routing = (target_range[:, :, None] == group_index[None, None, :]).astype(BF16)
    grads = jnp.einsum("roh,hrkw->orkw", routing, grads, preferred_element_type=F32).astype(BF16)
    weighted = (
        lax.dot_general(
            grads.reshape(-1, key_width),
            key_rows,
            (((1,), (1,)), ((), ())),
            preferred_element_type=F32,
        )
        * own_gain
    )

    embed_parts = [dot(rows, merger) for rows in merged_all]
    received = [[shift(part.astype(BF16), k) for k in others] for part in embed_parts]
    block_owner = (owners[:, None] == group_index[None, :]).astype(jnp.int32)
    block_range = jnp.sum(block_owner * target_range[0][None, :], axis=-1)
    received, late_blocks, early_terms = barrier((received, text_blocks[1], early_terms))
    embedded, sums, outgoing = features(
        parts, groups, owners, block_range, embed_parts, received, weighted, own_gain, key_rows
    )
    sums = lax.all_to_all(sums, "ctx", 0, 0, tiled=True)
    late_terms = text_terms(late_blocks)
    returned = [text_return(early_terms), text_return(late_terms)]
    sums, outgoing = barrier((sums, outgoing))
    arrived = lax.all_to_all(outgoing, "ctx", 0, 0, tiled=True)
    merger_grad, scales = finish(groups, float(width), owners, sums, embedded, weighted, merged_all)
    rotated = keys_out(
        parts,
        groups,
        index,
        image_grid,
        image_start,
        [early_terms, late_terms],
        returned,
        arrived,
        scales,
        cosine,
        sines,
    )
    return (rotated[None], merger_grad)


def solution(mesh):
    return jax.shard_map(
        on_device,
        mesh=mesh,
        in_specs=(
            P("dp", "ctx", None),
            P(),
            P("dp", None),
            P("dp", None),
            P("dp", "ctx"),
            P("dp", "ctx", None),
            P(),
            P("dp", None),
            P("dp", "ctx", None),
            P("dp", None, None),
            P("dp", None),
        ),
        out_specs=(P("dp", "ctx", None), P("dp", "ctx")),
        check_vma=False,
    )
```

```python
import math

import jax
import jax.numpy as jnp
from jax import lax
from jax.experimental import pallas as pl
from jax.experimental.pallas import tpu as pltpu
from jax.sharding import PartitionSpec as P


VHD = 80
HD = 128
EPS = 1e-06
THETA = 1000000.0
HIGHEST = lax.Precision.HIGHEST
BF16 = jnp.bfloat16
barrier = lax.optimization_barrier
F32 = jnp.float32


def layer_norm(values):
    average = jnp.mean(values, axis=-1, keepdims=True)
    centered = values - average
    variance = jnp.mean(centered * centered, axis=-1, keepdims=True)
    return centered * lax.rsqrt(variance + EPS)


def dot(a, b, **kw):
    return jnp.dot(a, b, preferred_element_type=F32, **kw)


def shift(x, k):
    size = lax.axis_size("dp")
    return lax.ppermute(x, "dp", [(i, (i + k) % size) for i in range(size)])


def gather_dp(x):
    return [x] + [shift(x, k) for k in range(1, lax.axis_size("dp"))]


def strides_of(size):
    return [1 << b for b in reversed(range(size.bit_length() - 1))]


def xor_gather(x, strides):
    size = lax.axis_size("ctx")
    pieces = [x]
    offsets = [[0]]
    for stride in strides:
        known = [o for piece in offsets for o in piece]
        joined = pieces[0] if len(pieces) == 1 else jnp.concatenate(pieces, axis=0)
        pieces.append(lax.ppermute(joined, "ctx", [(i, i ^ stride) for i in range(size)]))
        offsets.append([o ^ stride for o in known])
    return pieces, offsets


def gather_halves(x):
    size = lax.axis_size("ctx")
    own = lax.axis_index("ctx")
    if size & (size - 1) or size < 8:
        return [lax.all_gather(x, "ctx", axis=0, tiled=True)], jnp.arange(size, dtype=jnp.int32)
    strides = strides_of(size)
    middle = x.shape[1] // 2
    left, offsets = xor_gather(x[:, :middle], strides[:-1])
    right, others = xor_gather(x[:, middle:], strides[-2:-1] + strides[:-2])
    order = [o for piece in offsets for o in piece]
    rows = x.shape[0]
    found = {
        o: piece[j * rows : (j + 1) * rows]
        for piece, known in zip(right, others)
        for j, o in enumerate(known)
    }
    low = jnp.concatenate(
        [jnp.concatenate(left, axis=0), jnp.concatenate([found[o] for o in order], axis=0)], axis=1
    )
    high = lax.ppermute(low, "ctx", [(i, i ^ 1) for i in range(size)])
    order = order + [o ^ 1 for o in order]
    return [low, high], own ^ jnp.asarray(order, jnp.int32)


def find_image(own, tokens, grid_ref, start_ref, groups):
    zero = jnp.int32(0)
    first, cols, count, owner = zero, zero, zero, zero
    for o in range(groups):
        start = start_ref[0, o]
        here = (start >= own * tokens) & (start < (own + 1) * tokens)
        first = jnp.where(here, start, first)
        cols = jnp.where(here, grid_ref[0, o, 1], cols)
        count = jnp.where(here, grid_ref[0, o, 0] * grid_ref[0, o, 1], count)
        owner = jnp.where(here, o, owner)
    return first, cols, count, owner


SMEM = pl.BlockSpec(memory_space=pltpu.SMEM)
VMEM = pl.BlockSpec(memory_space=pltpu.VMEM)


def call(kernel, outs, ins, scalars=0, scratch=()):
    return pl.pallas_call(
        kernel,
        out_shape=outs,
        in_specs=[SMEM] * scalars + [VMEM] * (len(ins) - scalars),
        out_specs=[VMEM] * len(outs),
        scratch_shapes=list(scratch),
    )(*ins)


def project(parts, index, images, gain, weight):
    rows, _ = images[0].shape
    depth, columns = weight.shape
    third = columns // 3
    block = third // parts

    def kernel(index_ref, *refs):
        image_refs = refs[:parts]
        gain_ref, weight_ref, mine_ref, sent_ref = refs[parts:]
        own = index_ref[0]
        pieces = []
        for r in range(parts):
            normed = layer_norm(image_refs[r][...].astype(F32)) * gain_ref[...]
            piece = normed[:, :depth]
            for b in range(1, parts):
                piece = jnp.where(own == b, normed[:, b * depth : (b + 1) * depth], piece)
            pieces.append(piece.astype(BF16))
        product = dot(jnp.concatenate(pieces, axis=0), weight_ref[...])
        for b in range(parts):
            heads = jnp.concatenate(
                [product[:, j * third + b * block : j * third + (b + 1) * block] for j in range(3)],
                axis=1,
            )

            @pl.when(own == b)
            def _():
                mine_ref[...] = heads.reshape(parts, rows, 3 * block)

            for k in range(1, parts):

                @pl.when((own + k) % parts == b)
                def _():
                    for r in range(parts):
                        sent_ref[k - 1, (r + k) % parts] = heads[r * rows : (r + 1) * rows].astype(
                            BF16
                        )

    return call(
        kernel,
        (
            jax.ShapeDtypeStruct((parts, rows, 3 * block), F32),
            jax.ShapeDtypeStruct((parts - 1, parts, rows, 3 * block), BF16),
        ),
        (index, *images, gain, weight),
        scalars=1,
    )


def attend(parts, places, scalars, mine, received, images, out_weight):
    rows, width = images[0].shape
    capacity = rows // 4
    block = out_weight.shape[0]
    heads = block // VHD
    taken = places * capacity

    def kernel(scalar_ref, *refs):
        mine_ref = refs[0]
        received_refs = refs[1:parts]
        image_refs = refs[parts : 2 * parts]
        weight_ref, hidden_ref, sent_ref, scratch = refs[2 * parts :]
        own = scalar_ref[0]
        lane = lax.broadcasted_iota(jnp.int32, (rows, block), 1)
        key_slot = lax.broadcasted_iota(jnp.int32, (heads * rows, rows), 1) % capacity
        attended = []
        for r in range(parts):
            total = mine_ref[r]
            for ref in received_refs:
                total = total + ref[r].astype(F32)
            total = total.astype(BF16)
            queries = total[:, :block]
            keys = total[:, block : 2 * block]
            contents = total[:, 2 * block :]
            in_head = [(lane >= h * VHD) & (lane < (h + 1) * VHD) for h in range(heads)]
            stacked = jnp.concatenate(
                [jnp.where(inside, queries, jnp.zeros_like(queries)) for inside in in_head], axis=0
            )
            scores = lax.dot_general(
                stacked, keys, (((1,), (1,)), ((), ())), preferred_element_type=F32
            ) / math.sqrt(VHD)
            alive = (key_slot < scalar_ref[1 + r]).astype(F32)
            weights = jnp.exp(scores) * alive
            probability = (weights / jnp.sum(weights, axis=-1, keepdims=True)).astype(BF16)
            spread = dot(probability, contents)
            picked = jnp.where(in_head[0], spread[:rows], 0.0)
            for h in range(1, heads):
                picked = picked + jnp.where(in_head[h], spread[h * rows : (h + 1) * rows], 0.0)
            attended.append(picked.astype(BF16))
        product = dot(jnp.concatenate(attended, axis=0), weight_ref[...])
        scratch[...] = product.reshape(parts, rows, width)

        def start(index):
            return pl.multiple_of((index * 4 // parts) * capacity, capacity)

        for r in range(parts):
            at = pl.ds(start(own), taken)
            hidden_ref[r] = scratch[r, at, :] + image_refs[r][at, :].astype(F32)
            for k in range(1, parts):
                at = pl.ds(start((own + k) % parts), taken)
                sent_ref[k - 1, (r + k) % parts] = scratch[r, at, :].astype(BF16)

    return call(
        kernel,
        (
            jax.ShapeDtypeStruct((parts, taken, width), F32),
            jax.ShapeDtypeStruct((parts - 1, parts, taken, width), BF16),
        ),
        (scalars, mine, *received, *images, out_weight),
        scalars=1,
        scratch=[pltpu.VMEM((parts, rows, width), F32)],
    )


def features(parts, groups, owners, holders, own_parts, received, weighted, gain, key_rows):
    total = sum(p.shape[0] for p in own_parts)
    columns = own_parts[0].shape[1]
    rows = total // groups
    capacity = rows // parts
    key_width = key_rows.shape[1]
    chunks = len(own_parts)
    per_chunk = groups // chunks
    flat = [r for group in received for r in group]

    def kernel(owner_ref, holder_ref, *refs):
        part_refs = refs[:chunks]
        received_refs = refs[chunks : chunks + len(flat)]
        weighted_ref, gain_ref, key_ref, embed_ref, sums_ref, keys_ref, squared, multiplied = refs[
            chunks + len(flat) :
        ]
        picked = []
        for i in range(groups):
            chunk, base = i // per_chunk, (i % per_chunk) * rows
            block = part_refs[chunk][base : base + rows, :]
            for k in range(1, parts):
                ref = received_refs[chunk * (parts - 1) + k - 1]
                block = block + jnp.concatenate(
                    [
                        ref[pl.ds(base + (r - k) % parts * capacity, capacity), :].astype(F32)
                        for r in range(parts)
                    ],
                    axis=0,
                )
            block = block.astype(BF16)
            picked.append((block[:capacity].astype(F32) * gain_ref[...]).astype(BF16))
            embed_ref[pl.ds(i * rows, rows), :] = block
            values = block.astype(F32)
            at = pl.ds(pl.multiple_of(owner_ref[i] * rows, rows), rows)
            squared[at, :] = values * values
            multiplied[at, :] = values * weighted_ref[pl.ds(i * rows, rows), :]
        ones = jnp.ones((8, columns), F32)
        both = [
            lax.dot_general(
                ones,
                ref[...],
                (((1,), (1,)), ((), ())),
                precision=HIGHEST,
                preferred_element_type=F32,
            )[0:1]
            for ref in (squared, multiplied)
        ]
        for i in range(groups):
            sums_ref[i, :, 0:total] = both[0]
            sums_ref[i, :, total : 2 * total] = both[1]
        terms = dot(jnp.concatenate(picked, axis=0), key_ref[...]).astype(BF16)
        for i in range(groups):
            keys_ref[holder_ref[i]] = terms[i * capacity : (i + 1) * capacity]

    return call(
        kernel,
        (
            jax.ShapeDtypeStruct((total, columns), BF16),
            jax.ShapeDtypeStruct((groups, 1, 2 * total), F32),
            jax.ShapeDtypeStruct((groups, capacity, key_width), BF16),
        ),
        (owners, holders, *own_parts, *flat, weighted, gain, key_rows),
        scalars=2,
        scratch=[pltpu.VMEM((total, columns), F32), pltpu.VMEM((total, columns), F32)],
    )


def norm_scales(groups, width, owners, sums):
    total = sums.shape[2] // 2
    rows = total // groups

    def kernel(owner_ref, sums_ref, scale_ref, columns_ref, turned):
        whole = jnp.sum(sums_ref[...], axis=0)
        scale = lax.rsqrt(whole[:, :total] / width + EPS)
        slope = scale**3 * whole[:, total:] / width
        line = lax.broadcasted_iota(jnp.int32, (8, total), 0)
        both = jnp.where(line == 0, scale, slope)
        scale_ref[...] = both
        turned[...] = jnp.transpose(both)
        for i in range(groups):
            columns_ref[pl.ds(i * rows, rows), :] = turned[
                pl.ds(pl.multiple_of(owner_ref[i] * rows, rows), rows), :
            ]

    return call(
        kernel,
        (jax.ShapeDtypeStruct((8, total), F32), jax.ShapeDtypeStruct((total, 8), F32)),
        (owners, sums),
        scalars=1,
        scratch=[pltpu.VMEM((total, 8), F32)],
    )


def merge(parts, places, counts, hidden, received, extra):
    taken, width = hidden.shape[1:]
    capacity = taken // places
    main = places * width

    def kernel(count_ref, *refs):
        hidden_ref, received_refs, extra_ref, out_ref = refs[0], refs[1:-2], refs[-2], refs[-1]
        slot = lax.broadcasted_iota(jnp.int32, (capacity, width), 0)
        for r in range(parts):
            total = hidden_ref[r]
            for ref in received_refs:
                total = total + ref[r].astype(F32)
            normed = layer_norm(total).astype(BF16)
            for p in range(places):
                kept = normed[p * capacity : (p + 1) * capacity]
                kept = jnp.where(slot < count_ref[r], kept, jnp.zeros_like(kept))
                out_ref[r * capacity : (r + 1) * capacity, p * width : (p + 1) * width] = kept
        out_ref[:, main:] = extra_ref[...]

    return call(
        kernel,
        (jax.ShapeDtypeStruct((parts * capacity, main + extra.shape[1]), BF16),),
        (counts, hidden, *received, extra),
        scalars=1,
    )[0]


def angle_table(tokens, groups, capacity, index, grid, start):
    half = HD // 2
    first_cut = HD // 8
    second_cut = first_cut + 3 * HD // 16
    inverse = THETA ** (-(2.0 * (jnp.arange(HD, dtype=jnp.int32) % half).astype(F32)) / HD)

    def kernel(index_ref, grid_ref, start_ref, inverse_ref, out_ref):
        own = index_ref[1]
        first, cols, count, _ = find_image(own, tokens, grid_ref, start_ref, groups)
        line = lax.broadcasted_iota(jnp.int32, (tokens, HD), 0) + own * tokens
        frequency = lax.broadcasted_iota(jnp.int32, (tokens, HD), 1) % half
        inner = line - first
        row = jnp.zeros_like(inner)
        for j in range(1, capacity):
            row = row + (inner >= j * cols).astype(jnp.int32)
        offset = jnp.where(frequency < second_cut, row, inner - row * cols)
        offset = jnp.where(frequency < first_cut, 0, offset)
        inside = (inner >= 0) & (inner < count)
        chosen = jnp.where(inside, first + offset, line)
        out_ref[...] = chosen.astype(F32) * inverse_ref[...]

    return call(
        kernel,
        (jax.ShapeDtypeStruct((tokens, HD), F32),),
        (index, grid, start, inverse.reshape(1, -1)),
        scalars=3,
    )[0]


def place_rows(tokens, own, first, count, shape, axis):
    token = lax.broadcasted_iota(jnp.int32, shape, axis)
    slot = lax.broadcasted_iota(jnp.int32, shape, 1 - axis)
    return ((token + own * tokens - first == slot) & (slot < count)).astype(F32)


def turn(values, cosine, sines):
    heads = []
    for h in range(values.shape[1] // HD):
        head = values[:, h * HD : (h + 1) * HD]
        heads.append(head * cosine + pltpu.roll(head, HD // 2, 1) * sines)
    return jnp.concatenate(heads, axis=1)


def image_grads(tokens, groups, capacity, index, grid, start, cotangent, cosine, sines):
    width = cotangent.shape[1]

    def kernel(index_ref, grid_ref, start_ref, cotangent_ref, cosine_ref, sine_ref, out_ref):
        own = index_ref[1]
        first, _, count, _ = find_image(own, tokens, grid_ref, start_ref, groups)
        lane = lax.broadcasted_iota(jnp.int32, (tokens, HD), 1)
        signed = jnp.where(lane < HD // 2, sine_ref[...], -sine_ref[...])
        grad = turn(cotangent_ref[...].astype(F32), cosine_ref[...], signed)
        chosen = place_rows(tokens, own, first, count, (capacity, tokens), 1)
        out_ref[...] = dot(chosen, grad, precision=HIGHEST).astype(BF16)

    return call(
        kernel,
        (jax.ShapeDtypeStruct((capacity, width), BF16),),
        (index, grid, start, cotangent, cosine, sines),
        scalars=3,
    )[0]


def keys_out(parts, groups, index, grid, start, text_keys, returned, arrived, scales, cosine, sines):
    tokens, width = returned[0][0].shape[0] * len(returned), text_keys[0].shape[1]
    capacity = arrived.shape[1]
    total = scales.shape[1]
    chunks = len(text_keys)
    chunk = tokens // chunks
    flat = [r for group in returned for r in group]

    def kernel(index_ref, grid_ref, start_ref, *refs):
        text_refs = refs[:chunks]
        returned_refs = refs[chunks : chunks + len(flat)]
        arrived_ref, scale_ref, cosine_ref, sine_ref, out_ref = refs[chunks + len(flat) :]
        own = index_ref[1]
        first, _, count, owner = find_image(own, tokens, grid_ref, start_ref, groups)
        shape = (capacity, total)
        lane = lax.broadcasted_iota(jnp.int32, shape, 1)
        slot = lax.broadcasted_iota(jnp.int32, shape, 0)
        wanted = lane == owner * (parts * capacity) + slot
        scale = jnp.sum(jnp.where(wanted, scale_ref[0:1, :], 0.0), axis=-1, keepdims=True)
        image = jnp.sum(arrived_ref[...].astype(F32), axis=0) * scale
        chosen = place_rows(tokens, own, first, count, (tokens, capacity), 0)
        placed = dot(chosen, image, precision=HIGHEST)
        token = lax.broadcasted_iota(jnp.int32, (tokens, width), 0) + own * tokens
        inside = (token >= first) & (token < first + count)
        lane = lax.broadcasted_iota(jnp.int32, (tokens, HD), 1)
        signed = jnp.where(lane < HD // 2, -sine_ref[...], sine_ref[...])
        rows = []
        for j in range(chunks):
            part = text_refs[j][0:chunk, :]
            for k in range(parts - 1):
                part = part + returned_refs[j * (parts - 1) + k][...].astype(F32)
            rows.append(part)
        keys = jnp.where(inside, placed, jnp.concatenate(rows, axis=0))
        out_ref[...] = turn(keys, cosine_ref[...], signed).astype(BF16)

    return call(
        kernel,
        (jax.ShapeDtypeStruct((tokens, width), BF16),),
        (index, grid, start, *text_keys, *flat, arrived, scales, cosine, sines),
        scalars=3,
    )[0]


def text_norm(parts, chunks, index, text, gain):
    tokens, width = text.shape
    step = 32 if tokens // chunks % 32 == 0 else tokens // chunks
    block = width // parts
    steps = tokens // chunks // step

    def kernel(index_ref, text_ref, gain_ref, *refs):
        out_refs, scratch = refs[:-1], refs[-1]
        values = text_ref[...].astype(F32)
        scale = lax.rsqrt(jnp.mean(values * values, axis=-1, keepdims=True) + EPS)
        scratch[...] = (values * scale * gain_ref[...]).astype(BF16)
        for j in range(chunks):

            @pl.when(pl.program_id(0) // steps == j)
            def _():
                for k in range(parts):
                    start = pl.multiple_of((index_ref[0] + k) % parts * block, block)
                    out_refs[j * parts + k][...] = scratch[:, pl.ds(start, block)]

    def place(j):
        return lambda g: (jnp.clip(g - j * steps, 0, steps - 1), 0)

    flat = pl.pallas_call(
        kernel,
        grid=(tokens // step,),
        out_shape=[jax.ShapeDtypeStruct((tokens // chunks, block), BF16)] * (chunks * parts),
        in_specs=[
            SMEM,
            pl.BlockSpec((step, width), lambda g: (g, 0)),
            pl.BlockSpec((1, width), lambda g: (0, 0)),
        ],
        out_specs=[
            pl.BlockSpec((step, block), place(j)) for j in range(chunks) for _ in range(parts)
        ],
        scratch_shapes=[pltpu.VMEM((step, width), BF16)],
        name="text_norm",
    )(index, text, gain)
    return [flat[j * parts : (j + 1) * parts] for j in range(chunks)]


def on_device(
    patches,
    vit_norm_gain,
    vit_qkv,
    vit_out,
    merger,
    text_embed,
    lang_norm_gain,
    key_weight,
    key_cotangent,
    image_grid,
    image_start,
):
    parts = lax.axis_size("dp")
    groups = lax.axis_size("ctx")
    own_part = lax.axis_index("dp")
    own = lax.axis_index("ctx")
    tokens, width = text_embed.shape[1:]
    vit_width = patches.shape[2]
    capacity = patches.shape[1] // 4
    key_width = key_weight.shape[1]
    feature_cols = merger.shape[1]
    gain_line = lang_norm_gain.reshape(1, -1)
    index = jnp.stack([own_part, own]).astype(jnp.int32)
    others = range(1, parts)

    row = jnp.arange(4 * capacity, dtype=jnp.int32)
    source_row = (row % capacity) * 4 + row // capacity
    order_rows = (source_row[:, None] == row[None, :]).astype(BF16)
    images = gather_dp(dot(order_rows, patches[0]).astype(BF16))

    info = jnp.concatenate([image_grid[0].T, image_start], axis=0)
    infos = jnp.stack(gather_dp(info))
    counts = infos[:, 0] * infos[:, 1]
    target_range = infos[:, 2] // tokens
    group_index = jnp.arange(groups, dtype=jnp.int32)
    own_counts = jnp.sum(jnp.where(group_index[None] == own, counts, 0), axis=1)

    chunks = 2
    text_blocks = text_norm(parts, chunks, index, text_embed[0], gain_line)

    mine, sent = project(parts, index, images, vit_norm_gain.reshape(1, -1), vit_qkv)

    sent, grid, start = barrier((sent, image_grid, image_start))
    received = [shift(sent[k - 1], k) for k in others]
    angles = angle_table(tokens, groups, capacity, index, grid, start)
    cosine, sines = jnp.cos(angles), jnp.sin(angles)
    grads = image_grads(
        tokens, groups, capacity, index, grid, start, key_cotangent[0], cosine, sines
    )
    grads = jnp.concatenate(gather_dp(grads), axis=0)

    places = max(1, 4 // parts)
    pieces = max(1, parts // 4)
    piece_width = vit_width // pieces
    scalars = jnp.concatenate([index[:1], own_counts])
    hidden_rows, sent = attend(parts, places, scalars, mine, received, images, vit_out)
    received = [shift(sent[k - 1], k) for k in others]
    received, text_blocks, key_source = barrier((received, text_blocks, key_weight))
    merged = merge(parts, places, own_counts, hidden_rows, received, grads)
    if pieces > 1:
        taken = lax.dynamic_slice_in_dim(merged, (own_part % pieces) * piece_width, piece_width, 1)
        merged = jnp.concatenate([taken, grads], axis=1)
    merged_all, owners = gather_halves(merged)
    main = places * piece_width
    grads = jnp.concatenate([rows[:, main:] for rows in merged_all], axis=0)

    part_features = width // parts
    own_start = own * feature_cols
    holder_part = own_start // part_features
    candidate = lax.dynamic_slice_in_dim(key_source, own_start % part_features, feature_cols, 0)
    key_rows = jnp.where(own_part == holder_part, candidate, jnp.zeros_like(candidate))
    held_by = [g * feature_cols // part_features for g in range(groups)]
    for k in others:
        pairs = [
            (held_by[g] * groups + g, (held_by[g] + k) % parts * groups + g) for g in range(groups)
        ]
        key_rows = key_rows + lax.ppermute(candidate, ("dp", "ctx"), pairs)
    own_gain = lax.dynamic_slice_in_dim(lang_norm_gain, own_start, feature_cols, 0).reshape(1, -1)

    def text_terms(blocks):
        rows = [blocks[0]] + [shift(blocks[k], k) for k in others]
        return dot(jnp.concatenate(rows, axis=0), key_weight)

    def text_return(terms):
        size = terms.shape[0] // parts
        return [shift(terms[k * size : (k + 1) * size].astype(BF16), -k) for k in others]

    early_terms = text_terms(text_blocks[0])

    grads = grads.reshape(groups, parts, capacity, key_width)
    block_owner = (owners[:, None] == group_index[None, :]).astype(jnp.int32)
    block_range = jnp.sum(block_owner[None] * target_range[:, None, :], axis=-1)
    routing = (block_range[:, :, None] == owners[None, None, :]).astype(BF16)
    grads = jnp.einsum("roi,irkw->orkw", routing, grads, preferred_element_type=F32).astype(BF16)
    weighted = (
        lax.dot_general(
            grads.reshape(-1, key_width),
            key_rows,
            (((1,), (1,)), ((), ())),
            preferred_element_type=F32,
        )
        * own_gain
    )

    embed_parts = [dot(rows[:, :main], merger) for rows in merged_all]
    joined = jnp.concatenate([rows[:, :main] for rows in merged_all], axis=0)
    received = [[shift(part.astype(BF16), k) for k in others] for part in embed_parts]
    received, late_blocks = barrier((received, text_blocks[1]))
    embedded, sums, outgoing = features(
        parts, groups, owners, block_range[0], embed_parts, received, weighted, own_gain, key_rows
    )
    sums = lax.all_to_all(sums, "ctx", 0, 0, tiled=True)
    late_terms = text_terms(late_blocks)
    arrived = lax.all_to_all(outgoing, "ctx", 0, 0, tiled=True)
    returned = [text_return(early_terms), text_return(late_terms)]
    scales, columns = norm_scales(groups, float(width), owners, sums)
    grad_embedded = columns[:, 0:1] * weighted - embedded.astype(F32) * columns[:, 1:2]
    grad_embedded = grad_embedded.astype(BF16)
    merger_grad = lax.dot_general(
        joined, grad_embedded, (((0,), (0,)), ((), ())), preferred_element_type=F32
    )
    rotated = keys_out(
        parts,
        groups,
        index,
        image_grid,
        image_start,
        [early_terms, late_terms],
        returned,
        arrived,
        scales,
        cosine,
        sines,
    )
    return (rotated[None], merger_grad)


def solution(mesh):
    return jax.shard_map(
        on_device,
        mesh=mesh,
        in_specs=(
            P("dp", "ctx", None),
            P(),
            P("dp", None),
            P("dp", None),
            P("dp", "ctx"),
            P("dp", "ctx", None),
            P(),
            P("dp", None),
            P("dp", "ctx", None),
            P("dp", None, None),
            P("dp", None),
        ),
        out_specs=(P("dp", "ctx", None), P("dp", "ctx")),
        check_vma=False,
    )
```

```python
import math

import jax
import jax.numpy as jnp
from jax import lax
from jax.experimental import pallas as pl
from jax.experimental.pallas import tpu as pltpu
from jax.sharding import PartitionSpec as P


VHD = 80
HD = 128
EPS = 1e-06
THETA = 1000000.0
HIGHEST = lax.Precision.HIGHEST
BF16 = jnp.bfloat16
barrier = lax.optimization_barrier
F32 = jnp.float32


def layer_norm(values):
    average = jnp.mean(values, axis=-1, keepdims=True)
    centered = values - average
    variance = jnp.mean(centered * centered, axis=-1, keepdims=True)
    return centered * lax.rsqrt(variance + EPS)


def dot(a, b, **kw):
    return jnp.dot(a, b, preferred_element_type=F32, **kw)


def shift(x, k):
    size = lax.axis_size("dp")
    return lax.ppermute(x, "dp", [(i, (i + k) % size) for i in range(size)])


def gather_dp(x):
    return [x] + [shift(x, k) for k in range(1, lax.axis_size("dp"))]


def strides_of(size):
    return [1 << b for b in reversed(range(size.bit_length() - 1))]


def xor_gather(x, strides):
    size = lax.axis_size("ctx")
    pieces = [x]
    offsets = [[0]]
    for stride in strides:
        known = [o for piece in offsets for o in piece]
        joined = pieces[0] if len(pieces) == 1 else jnp.concatenate(pieces, axis=0)
        pieces.append(lax.ppermute(joined, "ctx", [(i, i ^ stride) for i in range(size)]))
        offsets.append([o ^ stride for o in known])
    return pieces, offsets


def gather_halves(left, right, main):
    size = lax.axis_size("ctx")
    own = lax.axis_index("ctx")
    middle, rows = left.shape[1], left.shape[0]
    if size & (size - 1) or size < 8:
        x = jnp.concatenate([left, right], axis=1)
        x = lax.all_gather(x, "ctx", axis=0, tiled=True)
        return [x[:, :main]], [x[:, main:]], jnp.arange(size, dtype=jnp.int32)
    strides = strides_of(size)
    lefts, offsets = xor_gather(left, strides[:-1])
    rights, others = xor_gather(right, strides[-2:-1] + strides[:-2])
    order = [o for piece in offsets for o in piece]
    found = {
        o: piece[j * rows : (j + 1) * rows]
        for piece, known in zip(rights, others)
        for j, o in enumerate(known)
    }
    rights = jnp.concatenate([found[o] for o in order], axis=0)
    low = jnp.concatenate([jnp.concatenate(lefts, axis=0), rights[:, : main - middle]], axis=1)
    rest = rights[:, main - middle :]
    pairs = [(i, i ^ 1) for i in range(size)]
    lows = [low, lax.ppermute(low, "ctx", pairs)]
    rests = [rest, lax.ppermute(rest, "ctx", pairs)]
    order = order + [o ^ 1 for o in order]
    return lows, rests, own ^ jnp.asarray(order, jnp.int32)


def find_image(own, tokens, grid_ref, start_ref, groups):
    zero = jnp.int32(0)
    first, cols, count, owner = zero, zero, zero, zero
    for o in range(groups):
        start = start_ref[0, o]
        here = (start >= own * tokens) & (start < (own + 1) * tokens)
        first = jnp.where(here, start, first)
        cols = jnp.where(here, grid_ref[0, o, 1], cols)
        count = jnp.where(here, grid_ref[0, o, 0] * grid_ref[0, o, 1], count)
        owner = jnp.where(here, o, owner)
    return first, cols, count, owner


SMEM = pl.BlockSpec(memory_space=pltpu.SMEM)
VMEM = pl.BlockSpec(memory_space=pltpu.VMEM)


def call(kernel, outs, ins, scalars=0, scratch=()):
    return pl.pallas_call(
        kernel,
        out_shape=outs,
        in_specs=[SMEM] * scalars + [VMEM] * (len(ins) - scalars),
        out_specs=[VMEM] * len(outs),
        scratch_shapes=list(scratch),
    )(*ins)


def project(parts, index, images, gain, weight):
    rows, _ = images[0].shape
    depth, columns = weight.shape
    third = columns // 3
    block = third // parts

    def kernel(index_ref, *refs):
        image_refs = refs[:parts]
        gain_ref, weight_ref, mine_ref, sent_ref = refs[parts:]
        own = index_ref[0]
        pieces = []
        for r in range(parts):
            normed = layer_norm(image_refs[r][...].astype(F32)) * gain_ref[...]
            piece = normed[:, :depth]
            for b in range(1, parts):
                piece = jnp.where(own == b, normed[:, b * depth : (b + 1) * depth], piece)
            pieces.append(piece.astype(BF16))
        product = dot(jnp.concatenate(pieces, axis=0), weight_ref[...])
        for b in range(parts):
            heads = jnp.concatenate(
                [product[:, j * third + b * block : j * third + (b + 1) * block] for j in range(3)],
                axis=1,
            )

            @pl.when(own == b)
            def _():
                mine_ref[...] = heads.reshape(parts, rows, 3 * block)

            for k in range(1, parts):

                @pl.when((own + k) % parts == b)
                def _():
                    for r in range(parts):
                        sent_ref[k - 1, (r + k) % parts] = heads[r * rows : (r + 1) * rows].astype(
                            BF16
                        )

    return call(
        kernel,
        (
            jax.ShapeDtypeStruct((parts, rows, 3 * block), F32),
            jax.ShapeDtypeStruct((parts - 1, parts, rows, 3 * block), BF16),
        ),
        (index, *images, gain, weight),
        scalars=1,
    )


def attend(parts, places, scalars, mine, received, images, out_weight):
    rows, width = images[0].shape
    capacity = rows // 4
    block = out_weight.shape[0]
    heads = block // VHD
    taken = places * capacity

    def kernel(scalar_ref, *refs):
        mine_ref = refs[0]
        received_refs = refs[1:parts]
        image_refs = refs[parts : 2 * parts]
        weight_ref, hidden_ref, sent_ref, scratch = refs[2 * parts :]
        own = scalar_ref[0]
        lane = lax.broadcasted_iota(jnp.int32, (rows, block), 1)
        key_slot = lax.broadcasted_iota(jnp.int32, (heads * rows, rows), 1) % capacity
        attended = []
        for r in range(parts):
            total = mine_ref[r]
            for ref in received_refs:
                total = total + ref[r].astype(F32)
            total = total.astype(BF16)
            queries = total[:, :block]
            keys = total[:, block : 2 * block]
            contents = total[:, 2 * block :]
            in_head = [(lane >= h * VHD) & (lane < (h + 1) * VHD) for h in range(heads)]
            stacked = jnp.concatenate(
                [jnp.where(inside, queries, jnp.zeros_like(queries)) for inside in in_head], axis=0
            )
            scores = lax.dot_general(
                stacked, keys, (((1,), (1,)), ((), ())), preferred_element_type=F32
            ) / math.sqrt(VHD)
            alive = (key_slot < scalar_ref[1 + r]).astype(F32)
            weights = jnp.exp(scores) * alive
            probability = (weights / jnp.sum(weights, axis=-1, keepdims=True)).astype(BF16)
            spread = dot(probability, contents)
            picked = jnp.where(in_head[0], spread[:rows], 0.0)
            for h in range(1, heads):
                picked = picked + jnp.where(in_head[h], spread[h * rows : (h + 1) * rows], 0.0)
            attended.append(picked.astype(BF16))
        product = dot(jnp.concatenate(attended, axis=0), weight_ref[...])
        scratch[...] = product.reshape(parts, rows, width)

        def start(index):
            return pl.multiple_of((index * 4 // parts) * capacity, capacity)

        for r in range(parts):
            at = pl.ds(start(own), taken)
            hidden_ref[r] = scratch[r, at, :] + image_refs[r][at, :].astype(F32)
            for k in range(1, parts):
                at = pl.ds(start((own + k) % parts), taken)
                sent_ref[k - 1, (r + k) % parts] = scratch[r, at, :].astype(BF16)

    return call(
        kernel,
        (
            jax.ShapeDtypeStruct((parts, taken, width), F32),
            jax.ShapeDtypeStruct((parts - 1, parts, taken, width), BF16),
        ),
        (scalars, mine, *received, *images, out_weight),
        scalars=1,
        scratch=[pltpu.VMEM((parts, rows, width), F32)],
    )


def features(parts, groups, owners, holders, own_parts, received, weighted, gain, key_rows):
    total = sum(p.shape[0] for p in own_parts)
    columns = own_parts[0].shape[1]
    rows = total // groups
    capacity = rows // parts
    key_width = key_rows.shape[1]
    chunks = len(own_parts)
    per_chunk = groups // chunks
    sum_rows = -(-6 * (total // key_width) // 8) * 8
    flat = [r for group in received for r in group]

    def kernel(owner_ref, holder_ref, *refs):
        part_refs = refs[:chunks]
        received_refs = refs[chunks : chunks + len(flat)]
        weighted_ref, gain_ref, key_ref, embed_ref, keys_ref, squared, multiplied = refs[
            chunks + len(flat) :
        ]
        picked = []
        for i in range(groups):
            chunk, base = i // per_chunk, (i % per_chunk) * rows
            block = part_refs[chunk][base : base + rows, :]
            for k in range(1, parts):
                ref = received_refs[chunk * (parts - 1) + k - 1]
                block = block + jnp.concatenate(
                    [
                        ref[pl.ds(base + (r - k) % parts * capacity, capacity), :].astype(F32)
                        for r in range(parts)
                    ],
                    axis=0,
                )
            block = block.astype(BF16)
            picked.append((block[:capacity].astype(F32) * gain_ref[...]).astype(BF16))
            embed_ref[pl.ds(i * rows, rows), :] = block
            values = block.astype(F32)
            at = pl.ds(pl.multiple_of(owner_ref[i] * rows, rows), rows)
            squared[at, :] = values * values
            multiplied[at, :] = values * weighted_ref[pl.ds(i * rows, rows), :]
        ones = jnp.ones((8, columns), F32)
        both = [
            lax.dot_general(
                ones,
                ref[...],
                (((1,), (1,)), ((), ())),
                precision=HIGHEST,
                preferred_element_type=F32,
            )[0:1]
            for ref in (squared, multiplied)
        ]
        lines = []
        for _ in range(3):
            rounded = [v.astype(BF16).astype(F32) for v in both]
            both = [v - w for v, w in zip(both, rounded)]
            for v in rounded:
                lines += [v[:, j : j + key_width] for j in range(0, total, key_width)]
        lines += [jnp.zeros_like(lines[0])] * (sum_rows - len(lines))
        lines = jnp.concatenate(lines, axis=0).astype(BF16)
        terms = dot(jnp.concatenate(picked, axis=0), key_ref[...]).astype(BF16)
        for i in range(groups):
            keys_ref[holder_ref[i], 0:capacity] = terms[i * capacity : (i + 1) * capacity]
            keys_ref[i, capacity:] = lines

    return call(
        kernel,
        (
            jax.ShapeDtypeStruct((total, columns), BF16),
            jax.ShapeDtypeStruct((groups, capacity + sum_rows, key_width), BF16),
        ),
        (owners, holders, *own_parts, *flat, weighted, gain, key_rows),
        scalars=2,
        scratch=[pltpu.VMEM((total, columns), F32), pltpu.VMEM((total, columns), F32)],
    )


def norm_scales(parts, groups, width, owners, arrived, capacity):
    rows = parts * capacity
    total = groups * rows
    lines = total // arrived.shape[2]

    def kernel(owner_ref, sums_ref, scale_ref, columns_ref, turned):
        summed = jnp.sum(sums_ref[:, capacity:, :].astype(F32), axis=0)

        def whole(q):
            pieces = []
            for j in range(lines):
                at = [(2 * p + q) * lines + j for p in range(3)]
                pieces.append(sum(summed[r : r + 1] for r in at))
            return jnp.concatenate(pieces, axis=1)

        scale = lax.rsqrt(whole(0) / width + EPS)
        slope = scale**3 * whole(1) / width
        line = lax.broadcasted_iota(jnp.int32, (8, total), 0)
        both = jnp.where(line == 0, scale, slope)
        scale_ref[...] = both
        turned[...] = jnp.transpose(both)
        for i in range(groups):
            columns_ref[pl.ds(i * rows, rows), :] = turned[
                pl.ds(pl.multiple_of(owner_ref[i] * rows, rows), rows), :
            ]

    return call(
        kernel,
        (jax.ShapeDtypeStruct((8, total), F32), jax.ShapeDtypeStruct((total, 8), F32)),
        (owners, arrived),
        scalars=1,
        scratch=[pltpu.VMEM((total, 8), F32)],
    )


def merge(parts, places, counts, hidden, received, extras):
    taken, width = hidden.shape[1:]
    capacity = taken // places
    main = places * width
    middle = (main + extras[0].shape[1]) // 256 * 128
    rest = main + extras[0].shape[1] - middle
    count = len(received)

    def kernel(count_ref, *refs):
        hidden_ref, received_refs = refs[0], refs[1 : 1 + count]
        extra_refs, left_ref, right_ref = refs[1 + count : -2], refs[-2], refs[-1]

        def put(rows, column, values):
            split = min(max(middle - column, 0), values.shape[1])
            if split:
                left_ref[rows, column : column + split] = values[:, :split]
            if split < values.shape[1]:
                begin = column + split - middle
                right_ref[rows, begin : begin + values.shape[1] - split] = values[:, split:]

        slot = lax.broadcasted_iota(jnp.int32, (capacity, width), 0)
        for r in range(parts):
            rows = pl.ds(r * capacity, capacity)
            total = hidden_ref[r]
            for ref in received_refs:
                total = total + ref[r].astype(F32)
            normed = layer_norm(total).astype(BF16)
            for p in range(places):
                kept = normed[p * capacity : (p + 1) * capacity]
                put(rows, p * width, jnp.where(slot < count_ref[r], kept, jnp.zeros_like(kept)))
            put(rows, main, extra_refs[r][...])

    return call(
        kernel,
        (
            jax.ShapeDtypeStruct((parts * capacity, middle), BF16),
            jax.ShapeDtypeStruct((parts * capacity, rest), BF16),
        ),
        (counts, hidden, *received, *extras),
        scalars=1,
    )


def angle_table(tokens, groups, capacity, index, grid, start):
    half = HD // 2
    first_cut = HD // 8
    second_cut = first_cut + 3 * HD // 16
    inverse = THETA ** (-(2.0 * (jnp.arange(HD, dtype=jnp.int32) % half).astype(F32)) / HD)

    def kernel(index_ref, grid_ref, start_ref, inverse_ref, out_ref):
        own = index_ref[1]
        first, cols, count, _ = find_image(own, tokens, grid_ref, start_ref, groups)
        line = lax.broadcasted_iota(jnp.int32, (tokens, HD), 0) + own * tokens
        frequency = lax.broadcasted_iota(jnp.int32, (tokens, HD), 1) % half
        inner = line - first
        row = jnp.zeros_like(inner)
        for j in range(1, capacity):
            row = row + (inner >= j * cols).astype(jnp.int32)
        offset = jnp.where(frequency < second_cut, row, inner - row * cols)
        offset = jnp.where(frequency < first_cut, 0, offset)
        inside = (inner >= 0) & (inner < count)
        chosen = jnp.where(inside, first + offset, line)
        out_ref[...] = chosen.astype(F32) * inverse_ref[...]

    return call(
        kernel,
        (jax.ShapeDtypeStruct((tokens, HD), F32),),
        (index, grid, start, inverse.reshape(1, -1)),
        scalars=3,
    )[0]


def place_rows(tokens, own, first, count, shape, axis):
    token = lax.broadcasted_iota(jnp.int32, shape, axis)
    slot = lax.broadcasted_iota(jnp.int32, shape, 1 - axis)
    return ((token + own * tokens - first == slot) & (slot < count)).astype(F32)


def turn(values, cosine, sines):
    heads = []
    for h in range(values.shape[1] // HD):
        head = values[:, h * HD : (h + 1) * HD]
        heads.append(head * cosine + pltpu.roll(head, HD // 2, 1) * sines)
    return jnp.concatenate(heads, axis=1)


def image_grads(tokens, groups, capacity, index, grid, start, cotangent, cosine, sines):
    width = cotangent.shape[1]

    def kernel(index_ref, grid_ref, start_ref, cotangent_ref, cosine_ref, sine_ref, out_ref):
        own = index_ref[1]
        first, _, count, _ = find_image(own, tokens, grid_ref, start_ref, groups)
        lane = lax.broadcasted_iota(jnp.int32, (tokens, HD), 1)
        signed = jnp.where(lane < HD // 2, sine_ref[...], -sine_ref[...])
        grad = turn(cotangent_ref[...].astype(F32), cosine_ref[...], signed)
        chosen = place_rows(tokens, own, first, count, (capacity, tokens), 1)
        out_ref[...] = dot(chosen, grad, precision=HIGHEST).astype(BF16)

    return call(
        kernel,
        (jax.ShapeDtypeStruct((capacity, width), BF16),),
        (index, grid, start, cotangent, cosine, sines),
        scalars=3,
    )[0]


def keys_out(parts, groups, index, grid, start, text_keys, returned, arrived, scales, cosine, sines):
    tokens, width = cosine.shape[0], text_keys[0].shape[1]
    total = scales.shape[1]
    capacity = total // (parts * groups)
    chunks = len(text_keys)
    sizes = [t.shape[0] // parts for t in text_keys]
    flat = [r for group in returned for r in group]

    def kernel(index_ref, grid_ref, start_ref, *refs):
        text_refs = refs[:chunks]
        returned_refs = refs[chunks : chunks + len(flat)]
        arrived_ref, scale_ref, cosine_ref, sine_ref, out_ref = refs[chunks + len(flat) :]
        own = index_ref[1]
        first, _, count, owner = find_image(own, tokens, grid_ref, start_ref, groups)
        shape = (capacity, total)
        lane = lax.broadcasted_iota(jnp.int32, shape, 1)
        slot = lax.broadcasted_iota(jnp.int32, shape, 0)
        wanted = lane == owner * (parts * capacity) + slot
        scale = jnp.sum(jnp.where(wanted, scale_ref[0:1, :], 0.0), axis=-1, keepdims=True)
        image = jnp.sum(arrived_ref[:, 0:capacity, :].astype(F32), axis=0) * scale
        chosen = place_rows(tokens, own, first, count, (tokens, capacity), 0)
        placed = dot(chosen, image, precision=HIGHEST)
        token = lax.broadcasted_iota(jnp.int32, (tokens, width), 0) + own * tokens
        inside = (token >= first) & (token < first + count)
        lane = lax.broadcasted_iota(jnp.int32, (tokens, HD), 1)
        signed = jnp.where(lane < HD // 2, -sine_ref[...], sine_ref[...])
        rows = []
        for j in range(chunks):
            part = text_refs[j][0 : sizes[j], :]
            for k in range(parts - 1):
                part = part + returned_refs[j * (parts - 1) + k][...].astype(F32)
            rows.append(part)
        keys = jnp.where(inside, placed, jnp.concatenate(rows, axis=0))
        out_ref[...] = turn(keys, cosine_ref[...], signed).astype(BF16)

    return call(
        kernel,
        (jax.ShapeDtypeStruct((tokens, width), BF16),),
        (index, grid, start, *text_keys, *flat, arrived, scales, cosine, sines),
        scalars=3,
    )[0]


def text_norm(parts, sizes, index, text, gain):
    tokens, width = text.shape
    step = math.gcd(32, *sizes)
    block = width // parts
    steps = [size // step for size in sizes]
    begins = [sum(steps[:j]) for j in range(len(steps))]

    def kernel(index_ref, text_ref, gain_ref, *refs):
        out_refs, scratch = refs[:-1], refs[-1]
        values = text_ref[...].astype(F32)
        scale = lax.rsqrt(jnp.mean(values * values, axis=-1, keepdims=True) + EPS)
        scratch[...] = (values * scale * gain_ref[...]).astype(BF16)
        now = pl.program_id(0)
        for j in range(len(sizes)):

            @pl.when((now >= begins[j]) & (now < begins[j] + steps[j]))
            def _():
                for k in range(parts):
                    start = pl.multiple_of((index_ref[0] + k) % parts * block, block)
                    out_refs[j * parts + k][...] = scratch[:, pl.ds(start, block)]

    def place(j):
        return lambda g: (jnp.clip(g - begins[j], 0, steps[j] - 1), 0)

    flat = pl.pallas_call(
        kernel,
        grid=(tokens // step,),
        out_shape=[jax.ShapeDtypeStruct((size, block), BF16) for size in sizes for _ in range(parts)],
        in_specs=[
            SMEM,
            pl.BlockSpec((step, width), lambda g: (g, 0)),
            pl.BlockSpec((1, width), lambda g: (0, 0)),
        ],
        out_specs=[
            pl.BlockSpec((step, block), place(j)) for j in range(len(sizes)) for _ in range(parts)
        ],
        scratch_shapes=[pltpu.VMEM((step, width), BF16)],
        name="text_norm",
    )(index, text, gain)
    return [flat[j * parts : (j + 1) * parts] for j in range(len(sizes))]


def on_device(
    patches,
    vit_norm_gain,
    vit_qkv,
    vit_out,
    merger,
    text_embed,
    lang_norm_gain,
    key_weight,
    key_cotangent,
    image_grid,
    image_start,
):
    parts = lax.axis_size("dp")
    groups = lax.axis_size("ctx")
    own_part = lax.axis_index("dp")
    own = lax.axis_index("ctx")
    tokens, width = text_embed.shape[1:]
    vit_width = patches.shape[2]
    capacity = patches.shape[1] // 4
    key_width = key_weight.shape[1]
    feature_cols = merger.shape[1]
    gain_line = lang_norm_gain.reshape(1, -1)
    index = jnp.stack([own_part, own]).astype(jnp.int32)
    others = range(1, parts)

    row = jnp.arange(4 * capacity, dtype=jnp.int32)
    source_row = (row % capacity) * 4 + row // capacity
    order_rows = (source_row[:, None] == row[None, :]).astype(BF16)
    images = gather_dp(dot(order_rows, patches[0]).astype(BF16))

    info = jnp.concatenate([image_grid[0].T, image_start], axis=0)
    infos = jnp.stack(gather_dp(info))
    counts = infos[:, 0] * infos[:, 1]
    target_range = infos[:, 2] // tokens
    group_index = jnp.arange(groups, dtype=jnp.int32)
    own_counts = jnp.sum(jnp.where(group_index[None] == own, counts, 0), axis=1)

    sizes = [tokens - tokens // 4, tokens // 4]
    text_blocks = text_norm(parts, sizes, index, text_embed[0], gain_line)

    mine, sent = project(parts, index, images, vit_norm_gain.reshape(1, -1), vit_qkv)

    sent, grid, start = barrier((sent, image_grid, image_start))
    received = [shift(sent[k - 1], k) for k in others]
    angles = angle_table(tokens, groups, capacity, index, grid, start)
    cosine, sines = jnp.cos(angles), jnp.sin(angles)
    grads = image_grads(
        tokens, groups, capacity, index, grid, start, key_cotangent[0], cosine, sines
    )
    grads = gather_dp(grads)

    places = max(1, 4 // parts)
    pieces = max(1, parts // 4)
    piece_width = vit_width // pieces
    scalars = jnp.concatenate([index[:1], own_counts])
    hidden_rows, sent = attend(parts, places, scalars, mine, received, images, vit_out)
    received = [shift(sent[k - 1], k) for k in others]
    received, text_blocks = barrier((received, text_blocks))
    left, right = merge(parts, places, own_counts, hidden_rows, received, grads)
    main = places * piece_width
    if pieces > 1:
        merged = jnp.concatenate([left, right], axis=1)
        begin = (own_part % pieces) * piece_width
        taken = lax.dynamic_slice_in_dim(merged[:, :vit_width], begin, piece_width, 1)
        merged = jnp.concatenate([taken, merged[:, vit_width:]], axis=1)
        middle = min(merged.shape[1] // 2, main)
        left, right = merged[:, :middle], merged[:, middle:]
    merged_all, grads, owners = gather_halves(left, right, main)

    part_features = width // parts
    own_start = own * feature_cols
    holder_part = own_start // part_features
    candidate = lax.dynamic_slice_in_dim(key_weight, own_start % part_features, feature_cols, 0)
    key_rows = jnp.where(own_part == holder_part, candidate, jnp.zeros_like(candidate))
    held_by = [g * feature_cols // part_features for g in range(groups)]
    for k in others:
        pairs = [
            (held_by[g] * groups + g, (held_by[g] + k) % parts * groups + g) for g in range(groups)
        ]
        key_rows = key_rows + lax.ppermute(candidate, ("dp", "ctx"), pairs)
    own_gain = lax.dynamic_slice_in_dim(lang_norm_gain, own_start, feature_cols, 0).reshape(1, -1)

    def text_terms(blocks):
        rows = [blocks[0]] + [shift(blocks[k], k) for k in others]
        return dot(jnp.concatenate(rows, axis=0), key_weight)

    def text_return(terms):
        size = terms.shape[0] // parts
        return [shift(terms[k * size : (k + 1) * size].astype(BF16), -k) for k in others]

    early_terms = text_terms(text_blocks[0])

    grads = jnp.concatenate(grads, axis=0).reshape(groups, parts, capacity, key_width)
    block_owner = (owners[:, None] == group_index[None, :]).astype(jnp.int32)
    block_range = jnp.sum(block_owner[None] * target_range[:, None, :], axis=-1)
    routing = (block_range[:, :, None] == owners[None, None, :]).astype(BF16)
    grads = jnp.einsum("roi,irkw->orkw", routing, grads, preferred_element_type=F32).astype(BF16)
    weighted = (
        lax.dot_general(
            grads.reshape(-1, key_width),
            key_rows,
            (((1,), (1,)), ((), ())),
            preferred_element_type=F32,
        )
        * own_gain
    )

    embed_parts = [dot(rows, merger) for rows in merged_all]
    joined = jnp.concatenate(merged_all, axis=0)
    received = [[shift(part.astype(BF16), k) for k in others] for part in embed_parts]
    received, late_blocks = barrier((received, text_blocks[1]))
    embedded, outgoing = features(
        parts, groups, owners, block_range[0], embed_parts, received, weighted, own_gain, key_rows
    )
    arrived = lax.all_to_all(outgoing, "ctx", 0, 0, tiled=True)
    late_terms = text_terms(late_blocks)
    returned = [text_return(early_terms), text_return(late_terms)]
    scales, columns = norm_scales(
        parts, groups, float(width), owners, arrived, capacity
    )
    grad_embedded = columns[:, 0:1] * weighted - embedded.astype(F32) * columns[:, 1:2]
    grad_embedded = grad_embedded.astype(BF16)
    merger_grad = lax.dot_general(
        joined, grad_embedded, (((0,), (0,)), ((), ())), preferred_element_type=F32
    )
    rotated = keys_out(
        parts,
        groups,
        index,
        image_grid,
        image_start,
        [early_terms, late_terms],
        returned,
        arrived,
        scales,
        cosine,
        sines,
    )
    return (rotated[None], merger_grad)


def solution(mesh):
    return jax.shard_map(
        on_device,
        mesh=mesh,
        in_specs=(
            P("dp", "ctx", None),
            P(),
            P("dp", None),
            P("dp", None),
            P("dp", "ctx"),
            P("dp", "ctx", None),
            P(),
            P("dp", None),
            P("dp", "ctx", None),
            P("dp", None, None),
            P("dp", None),
        ),
        out_specs=(P("dp", "ctx", None), P("dp", "ctx")),
        check_vma=False,
    )
```

```python
import math

import jax
import jax.numpy as jnp
from jax import lax
from jax.experimental import pallas as pl
from jax.experimental.pallas import tpu as pltpu
from jax.sharding import PartitionSpec as P


VHD = 80
HD = 128
EPS = 1e-06
THETA = 1000000.0
HIGHEST = lax.Precision.HIGHEST
BF16 = jnp.bfloat16
barrier = lax.optimization_barrier
F32 = jnp.float32


def layer_norm(values):
    average = jnp.mean(values, axis=-1, keepdims=True)
    centered = values - average
    variance = jnp.mean(centered * centered, axis=-1, keepdims=True)
    return centered * lax.rsqrt(variance + EPS)


def dot(a, b, **kw):
    return jnp.dot(a, b, preferred_element_type=F32, **kw)


def shift(x, k):
    size = lax.axis_size("dp")
    return lax.ppermute(x, "dp", [(i, (i + k) % size) for i in range(size)])


def gather_dp(x):
    return [x] + [shift(x, k) for k in range(1, lax.axis_size("dp"))]


def strides_of(size):
    return [1 << b for b in reversed(range(size.bit_length() - 1))]


def xor_gather(x, strides):
    size = lax.axis_size("ctx")
    pieces = [x]
    offsets = [[0]]
    for stride in strides:
        known = [o for piece in offsets for o in piece]
        joined = pieces[0] if len(pieces) == 1 else jnp.concatenate(pieces, axis=0)
        pieces.append(lax.ppermute(joined, "ctx", [(i, i ^ stride) for i in range(size)]))
        offsets.append([o ^ stride for o in known])
    return pieces, offsets


def gather_halves(left, right, main, own):
    size = lax.axis_size("ctx")
    middle, rows = left.shape[1], left.shape[0]
    if size & (size - 1) or size < 8:
        x = jnp.concatenate([left, right], axis=1)
        x = lax.all_gather(x, "ctx", axis=0, tiled=True)
        return [x[:, :main]], [x[:, main:]], jnp.arange(size, dtype=jnp.int32)
    strides = strides_of(size)
    lefts, offsets = xor_gather(left, strides[:-1])
    rights, others = xor_gather(right, strides[-2:-1] + strides[:-2])
    order = [o for piece in offsets for o in piece]
    found = {
        o: piece[j * rows : (j + 1) * rows]
        for piece, known in zip(rights, others)
        for j, o in enumerate(known)
    }
    rights = jnp.concatenate([found[o] for o in order], axis=0)
    low = jnp.concatenate([jnp.concatenate(lefts, axis=0), rights[:, : main - middle]], axis=1)
    rest = rights[:, main - middle :]
    low, own = barrier((low, own))
    pairs = [(i, i ^ 1) for i in range(size)]
    lows = [low, lax.ppermute(low, "ctx", pairs)]
    rests = [rest, lax.ppermute(rest, "ctx", pairs)]
    order = order + [o ^ 1 for o in order]
    return lows, rests, own ^ jnp.asarray(order, jnp.int32)


def find_image(own, tokens, grid_ref, start_ref, groups):
    zero = jnp.int32(0)
    first, cols, count, owner = zero, zero, zero, zero
    for o in range(groups):
        start = start_ref[0, o]
        here = (start >= own * tokens) & (start < (own + 1) * tokens)
        first = jnp.where(here, start, first)
        cols = jnp.where(here, grid_ref[0, o, 1], cols)
        count = jnp.where(here, grid_ref[0, o, 0] * grid_ref[0, o, 1], count)
        owner = jnp.where(here, o, owner)
    return first, cols, count, owner


SMEM = pl.BlockSpec(memory_space=pltpu.SMEM)
VMEM = pl.BlockSpec(memory_space=pltpu.VMEM)


def call(kernel, outs, ins, scalars=0, scratch=()):
    return pl.pallas_call(
        kernel,
        out_shape=outs,
        in_specs=[SMEM] * scalars + [VMEM] * (len(ins) - scalars),
        out_specs=[VMEM] * len(outs),
        scratch_shapes=list(scratch),
    )(*ins)


def project(parts, index, images, gain, weight):
    rows, _ = images[0].shape
    depth, columns = weight.shape
    third = columns // 3
    block = third // parts

    def kernel(index_ref, *refs):
        image_refs = refs[:parts]
        gain_ref, weight_ref, mine_ref, sent_ref = refs[parts:]
        own = index_ref[0]
        pieces = []
        for r in range(parts):
            normed = layer_norm(image_refs[r][...].astype(F32)) * gain_ref[...]
            piece = normed[:, :depth]
            for b in range(1, parts):
                piece = jnp.where(own == b, normed[:, b * depth : (b + 1) * depth], piece)
            pieces.append(piece.astype(BF16))
        product = dot(jnp.concatenate(pieces, axis=0), weight_ref[...])
        for b in range(parts):
            heads = jnp.concatenate(
                [product[:, j * third + b * block : j * third + (b + 1) * block] for j in range(3)],
                axis=1,
            )

            @pl.when(own == b)
            def _():
                mine_ref[...] = heads.reshape(parts, rows, 3 * block)

            for k in range(1, parts):

                @pl.when((own + k) % parts == b)
                def _():
                    for r in range(parts):
                        sent_ref[k - 1, (r + k) % parts] = heads[r * rows : (r + 1) * rows].astype(
                            BF16
                        )

    return call(
        kernel,
        (
            jax.ShapeDtypeStruct((parts, rows, 3 * block), F32),
            jax.ShapeDtypeStruct((parts - 1, parts, rows, 3 * block), BF16),
        ),
        (index, *images, gain, weight),
        scalars=1,
    )


def attend(parts, places, scalars, mine, received, images, out_weight):
    rows, width = images[0].shape
    capacity = rows // 4
    block = out_weight.shape[0]
    heads = block // VHD
    taken = places * capacity

    def kernel(scalar_ref, *refs):
        mine_ref = refs[0]
        received_refs = refs[1:parts]
        image_refs = refs[parts : 2 * parts]
        weight_ref, hidden_ref, sent_ref, scratch = refs[2 * parts :]
        own = scalar_ref[0]
        lane = lax.broadcasted_iota(jnp.int32, (rows, block), 1)
        key_slot = lax.broadcasted_iota(jnp.int32, (heads * rows, rows), 1) % capacity
        attended = []
        for r in range(parts):
            total = mine_ref[r]
            for ref in received_refs:
                total = total + ref[r].astype(F32)
            total = total.astype(BF16)
            queries = total[:, :block]
            keys = total[:, block : 2 * block]
            contents = total[:, 2 * block :]
            in_head = [(lane >= h * VHD) & (lane < (h + 1) * VHD) for h in range(heads)]
            stacked = jnp.concatenate(
                [jnp.where(inside, queries, jnp.zeros_like(queries)) for inside in in_head], axis=0
            )
            scores = lax.dot_general(
                stacked, keys, (((1,), (1,)), ((), ())), preferred_element_type=F32
            ) / math.sqrt(VHD)
            alive = (key_slot < scalar_ref[1 + r]).astype(F32)
            weights = jnp.exp(scores) * alive
            probability = (weights / jnp.sum(weights, axis=-1, keepdims=True)).astype(BF16)
            spread = dot(probability, contents)
            picked = jnp.where(in_head[0], spread[:rows], 0.0)
            for h in range(1, heads):
                picked = picked + jnp.where(in_head[h], spread[h * rows : (h + 1) * rows], 0.0)
            attended.append(picked.astype(BF16))
        product = dot(jnp.concatenate(attended, axis=0), weight_ref[...])
        scratch[...] = product.reshape(parts, rows, width)

        def start(index):
            return pl.multiple_of((index * 4 // parts) * capacity, capacity)

        for r in range(parts):
            at = pl.ds(start(own), taken)
            hidden_ref[r] = scratch[r, at, :] + image_refs[r][at, :].astype(F32)
            for k in range(1, parts):
                at = pl.ds(start((own + k) % parts), taken)
                sent_ref[k - 1, (r + k) % parts] = scratch[r, at, :].astype(BF16)

    return call(
        kernel,
        (
            jax.ShapeDtypeStruct((parts, taken, width), F32),
            jax.ShapeDtypeStruct((parts - 1, parts, taken, width), BF16),
        ),
        (scalars, mine, *received, *images, out_weight),
        scalars=1,
        scratch=[pltpu.VMEM((parts, rows, width), F32)],
    )


def features(parts, groups, owners, holders, own_parts, received, weighted, gain, key_rows):
    total = sum(p.shape[0] for p in own_parts)
    columns = own_parts[0].shape[1]
    rows = total // groups
    capacity = rows // parts
    key_width = key_rows.shape[1]
    chunks = len(own_parts)
    per_chunk = groups // chunks
    sum_rows = -(-6 * (total // key_width) // 8) * 8
    flat = [r for group in received for r in group]

    def kernel(owner_ref, holder_ref, *refs):
        part_refs = refs[:chunks]
        received_refs = refs[chunks : chunks + len(flat)]
        weighted_ref, gain_ref, key_ref, embed_ref, keys_ref, squared, multiplied = refs[
            chunks + len(flat) :
        ]
        picked = []
        for i in range(groups):
            chunk, base = i // per_chunk, (i % per_chunk) * rows
            block = part_refs[chunk][base : base + rows, :]
            for k in range(1, parts):
                ref = received_refs[chunk * (parts - 1) + k - 1]
                block = block + jnp.concatenate(
                    [
                        ref[pl.ds(base + (r - k) % parts * capacity, capacity), :].astype(F32)
                        for r in range(parts)
                    ],
                    axis=0,
                )
            block = block.astype(BF16)
            picked.append((block[:capacity].astype(F32) * gain_ref[...]).astype(BF16))
            embed_ref[pl.ds(i * rows, rows), :] = block
            values = block.astype(F32)
            at = pl.ds(pl.multiple_of(owner_ref[i] * rows, rows), rows)
            squared[at, :] = values * values
            multiplied[at, :] = values * weighted_ref[pl.ds(i * rows, rows), :]
        ones = jnp.ones((8, columns), F32)
        both = [
            lax.dot_general(
                ones,
                ref[...],
                (((1,), (1,)), ((), ())),
                precision=HIGHEST,
                preferred_element_type=F32,
            )[0:1]
            for ref in (squared, multiplied)
        ]
        lines = []
        for _ in range(3):
            rounded = [v.astype(BF16).astype(F32) for v in both]
            both = [v - w for v, w in zip(both, rounded)]
            for v in rounded:
                lines += [v[:, j : j + key_width] for j in range(0, total, key_width)]
        lines += [jnp.zeros_like(lines[0])] * (sum_rows - len(lines))
        lines = jnp.concatenate(lines, axis=0).astype(BF16)
        terms = dot(jnp.concatenate(picked, axis=0), key_ref[...]).astype(BF16)
        for i in range(groups):
            keys_ref[holder_ref[i], 0:capacity] = terms[i * capacity : (i + 1) * capacity]
            keys_ref[i, capacity:] = lines

    return call(
        kernel,
        (
            jax.ShapeDtypeStruct((total, columns), BF16),
            jax.ShapeDtypeStruct((groups, capacity + sum_rows, key_width), BF16),
        ),
        (owners, holders, *own_parts, *flat, weighted, gain, key_rows),
        scalars=2,
        scratch=[pltpu.VMEM((total, columns), F32), pltpu.VMEM((total, columns), F32)],
    )


def norm_scales(parts, groups, width, owners, arrived, embedded, weighted):
    total, columns = embedded.shape
    rows = total // groups
    capacity = rows // parts
    lines = total // arrived.shape[2]

    def kernel(owner_ref, sums_ref, embed_ref, weighted_ref, scale_ref, grad_ref, turned):
        summed = jnp.sum(sums_ref[:, capacity:, :].astype(F32), axis=0)

        def whole(q):
            pieces = []
            for j in range(lines):
                at = [(2 * p + q) * lines + j for p in range(3)]
                pieces.append(sum(summed[r : r + 1] for r in at))
            return jnp.concatenate(pieces, axis=1)

        scale = lax.rsqrt(whole(0) / width + EPS)
        slope = scale**3 * whole(1) / width
        line = lax.broadcasted_iota(jnp.int32, (8, total), 0)
        both = jnp.where(line == 0, scale, slope)
        scale_ref[...] = both
        turned[...] = jnp.transpose(both)
        for i in range(groups):
            at = pl.ds(i * rows, rows)
            both = turned[pl.ds(pl.multiple_of(owner_ref[i] * rows, rows), rows), :]
            grad = both[:, 0:1] * weighted_ref[at, :] - embed_ref[at, :].astype(F32) * both[:, 1:2]
            grad_ref[at, :] = grad.astype(BF16)

    return call(
        kernel,
        (jax.ShapeDtypeStruct((8, total), F32), jax.ShapeDtypeStruct((total, columns), BF16)),
        (owners, arrived, embedded, weighted),
        scalars=1,
        scratch=[pltpu.VMEM((total, 8), F32)],
    )


def merge(parts, places, counts, hidden, received, extras):
    taken, width = hidden.shape[1:]
    capacity = taken // places
    main = places * width
    middle = (main + extras[0].shape[1]) // 256 * 128
    rest = main + extras[0].shape[1] - middle
    count = len(received)

    def kernel(count_ref, *refs):
        hidden_ref, received_refs = refs[0], refs[1 : 1 + count]
        extra_refs, left_ref, right_ref = refs[1 + count : -2], refs[-2], refs[-1]

        def put(rows, column, values):
            split = min(max(middle - column, 0), values.shape[1])
            if split:
                left_ref[rows, column : column + split] = values[:, :split]
            if split < values.shape[1]:
                begin = column + split - middle
                right_ref[rows, begin : begin + values.shape[1] - split] = values[:, split:]

        slot = lax.broadcasted_iota(jnp.int32, (capacity, width), 0)
        for r in range(parts):
            rows = pl.ds(r * capacity, capacity)
            total = hidden_ref[r]
            for ref in received_refs:
                total = total + ref[r].astype(F32)
            normed = layer_norm(total).astype(BF16)
            for p in range(places):
                kept = normed[p * capacity : (p + 1) * capacity]
                put(rows, p * width, jnp.where(slot < count_ref[r], kept, jnp.zeros_like(kept)))
            put(rows, main, extra_refs[r][...])

    return call(
        kernel,
        (
            jax.ShapeDtypeStruct((parts * capacity, middle), BF16),
            jax.ShapeDtypeStruct((parts * capacity, rest), BF16),
        ),
        (counts, hidden, *received, *extras),
        scalars=1,
    )


def angle_table(tokens, groups, capacity, index, grid, start):
    half = HD // 2
    first_cut = HD // 8
    second_cut = first_cut + 3 * HD // 16
    inverse = THETA ** (-(2.0 * (jnp.arange(HD, dtype=jnp.int32) % half).astype(F32)) / HD)

    def kernel(index_ref, grid_ref, start_ref, inverse_ref, out_ref):
        own = index_ref[1]
        first, cols, count, _ = find_image(own, tokens, grid_ref, start_ref, groups)
        line = lax.broadcasted_iota(jnp.int32, (tokens, HD), 0) + own * tokens
        frequency = lax.broadcasted_iota(jnp.int32, (tokens, HD), 1) % half
        inner = line - first
        row = jnp.zeros_like(inner)
        for j in range(1, capacity):
            row = row + (inner >= j * cols).astype(jnp.int32)
        offset = jnp.where(frequency < second_cut, row, inner - row * cols)
        offset = jnp.where(frequency < first_cut, 0, offset)
        inside = (inner >= 0) & (inner < count)
        chosen = jnp.where(inside, first + offset, line)
        out_ref[...] = chosen.astype(F32) * inverse_ref[...]

    return call(
        kernel,
        (jax.ShapeDtypeStruct((tokens, HD), F32),),
        (index, grid, start, inverse.reshape(1, -1)),
        scalars=3,
    )[0]


def place_rows(tokens, own, first, count, shape, axis):
    token = lax.broadcasted_iota(jnp.int32, shape, axis)
    slot = lax.broadcasted_iota(jnp.int32, shape, 1 - axis)
    return ((token + own * tokens - first == slot) & (slot < count)).astype(F32)


def turn(values, cosine, sines):
    heads = []
    for h in range(values.shape[1] // HD):
        head = values[:, h * HD : (h + 1) * HD]
        heads.append(head * cosine + pltpu.roll(head, HD // 2, 1) * sines)
    return jnp.concatenate(heads, axis=1)


def image_grads(tokens, groups, capacity, index, grid, start, cotangent, cosine, sines):
    width = cotangent.shape[1]

    def kernel(index_ref, grid_ref, start_ref, cotangent_ref, cosine_ref, sine_ref, out_ref):
        own = index_ref[1]
        first, _, count, _ = find_image(own, tokens, grid_ref, start_ref, groups)
        lane = lax.broadcasted_iota(jnp.int32, (tokens, HD), 1)
        signed = jnp.where(lane < HD // 2, sine_ref[...], -sine_ref[...])
        grad = turn(cotangent_ref[...].astype(F32), cosine_ref[...], signed)
        chosen = place_rows(tokens, own, first, count, (capacity, tokens), 1)
        out_ref[...] = dot(chosen, grad, precision=HIGHEST).astype(BF16)

    return call(
        kernel,
        (jax.ShapeDtypeStruct((capacity, width), BF16),),
        (index, grid, start, cotangent, cosine, sines),
        scalars=3,
    )[0]


def keys_out(parts, groups, index, grid, start, text_keys, returned, arrived, scales, cosine, sines):
    tokens, width = cosine.shape[0], text_keys[0].shape[1]
    total = scales.shape[1]
    capacity = total // (parts * groups)
    chunks = len(text_keys)
    sizes = [t.shape[0] // parts for t in text_keys]
    flat = [r for group in returned for r in group]

    def kernel(index_ref, grid_ref, start_ref, *refs):
        text_refs = refs[:chunks]
        returned_refs = refs[chunks : chunks + len(flat)]
        arrived_ref, scale_ref, cosine_ref, sine_ref, out_ref = refs[chunks + len(flat) :]
        own = index_ref[1]
        first, _, count, owner = find_image(own, tokens, grid_ref, start_ref, groups)
        shape = (capacity, total)
        lane = lax.broadcasted_iota(jnp.int32, shape, 1)
        slot = lax.broadcasted_iota(jnp.int32, shape, 0)
        wanted = lane == owner * (parts * capacity) + slot
        scale = jnp.sum(jnp.where(wanted, scale_ref[0:1, :], 0.0), axis=-1, keepdims=True)
        image = jnp.sum(arrived_ref[:, 0:capacity, :].astype(F32), axis=0) * scale
        chosen = place_rows(tokens, own, first, count, (tokens, capacity), 0)
        placed = dot(chosen, image, precision=HIGHEST)
        token = lax.broadcasted_iota(jnp.int32, (tokens, width), 0) + own * tokens
        inside = (token >= first) & (token < first + count)
        lane = lax.broadcasted_iota(jnp.int32, (tokens, HD), 1)
        signed = jnp.where(lane < HD // 2, -sine_ref[...], sine_ref[...])
        rows = []
        for j in range(chunks):
            part = text_refs[j][0 : sizes[j], :]
            for k in range(parts - 1):
                part = part + returned_refs[j * (parts - 1) + k][...].astype(F32)
            rows.append(part)
        keys = jnp.where(inside, placed, jnp.concatenate(rows, axis=0))
        out_ref[...] = turn(keys, cosine_ref[...], signed).astype(BF16)

    return call(
        kernel,
        (jax.ShapeDtypeStruct((tokens, width), BF16),),
        (index, grid, start, *text_keys, *flat, arrived, scales, cosine, sines),
        scalars=3,
    )[0]


def text_norm(parts, sizes, index, text, gain):
    tokens, width = text.shape
    step = math.gcd(32, *sizes)
    block = width // parts
    steps = [size // step for size in sizes]
    begins = [sum(steps[:j]) for j in range(len(steps))]

    def kernel(index_ref, text_ref, gain_ref, *refs):
        out_refs, scratch = refs[:-1], refs[-1]
        values = text_ref[...].astype(F32)
        scale = lax.rsqrt(jnp.mean(values * values, axis=-1, keepdims=True) + EPS)
        scratch[...] = (values * scale * gain_ref[...]).astype(BF16)
        now = pl.program_id(0)
        for j in range(len(sizes)):

            @pl.when((now >= begins[j]) & (now < begins[j] + steps[j]))
            def _():
                for k in range(parts):
                    start = pl.multiple_of((index_ref[0] + k) % parts * block, block)
                    out_refs[j * parts + k][...] = scratch[:, pl.ds(start, block)]

    def place(j):
        return lambda g: (jnp.clip(g - begins[j], 0, steps[j] - 1), 0)

    flat = pl.pallas_call(
        kernel,
        grid=(tokens // step,),
        out_shape=[jax.ShapeDtypeStruct((size, block), BF16) for size in sizes for _ in range(parts)],
        in_specs=[
            SMEM,
            pl.BlockSpec((step, width), lambda g: (g, 0)),
            pl.BlockSpec((1, width), lambda g: (0, 0)),
        ],
        out_specs=[
            pl.BlockSpec((step, block), place(j)) for j in range(len(sizes)) for _ in range(parts)
        ],
        scratch_shapes=[pltpu.VMEM((step, width), BF16)],
        name="text_norm",
    )(index, text, gain)
    return [flat[j * parts : (j + 1) * parts] for j in range(len(sizes))]


def on_device(
    patches,
    vit_norm_gain,
    vit_qkv,
    vit_out,
    merger,
    text_embed,
    lang_norm_gain,
    key_weight,
    key_cotangent,
    image_grid,
    image_start,
):
    parts = lax.axis_size("dp")
    groups = lax.axis_size("ctx")
    own_part = lax.axis_index("dp")
    own = lax.axis_index("ctx")
    tokens, width = text_embed.shape[1:]
    vit_width = patches.shape[2]
    capacity = patches.shape[1] // 4
    key_width = key_weight.shape[1]
    feature_cols = merger.shape[1]
    gain_line = lang_norm_gain.reshape(1, -1)
    index = jnp.stack([own_part, own]).astype(jnp.int32)
    others = range(1, parts)

    row = jnp.arange(4 * capacity, dtype=jnp.int32)
    source_row = (row % capacity) * 4 + row // capacity
    order_rows = (source_row[:, None] == row[None, :]).astype(BF16)
    images = gather_dp(dot(order_rows, patches[0]).astype(BF16))

    info = jnp.concatenate([image_grid[0].T, image_start], axis=0)
    infos = jnp.stack(gather_dp(info))
    counts = infos[:, 0] * infos[:, 1]
    target_range = infos[:, 2] // tokens
    group_index = jnp.arange(groups, dtype=jnp.int32)
    own_counts = jnp.sum(jnp.where(group_index[None] == own, counts, 0), axis=1)

    sizes = [tokens - tokens // 4, tokens // 4]
    text_blocks = text_norm(parts, sizes, index, text_embed[0], gain_line)

    mine, sent = project(parts, index, images, vit_norm_gain.reshape(1, -1), vit_qkv)

    sent, grid, start = barrier((sent, image_grid, image_start))
    received = [shift(sent[k - 1], k) for k in others]
    angles = angle_table(tokens, groups, capacity, index, grid, start)
    cosine, sines = jnp.cos(angles), jnp.sin(angles)
    grads = image_grads(
        tokens, groups, capacity, index, grid, start, key_cotangent[0], cosine, sines
    )
    grads = gather_dp(grads)

    places = max(1, 4 // parts)
    pieces = max(1, parts // 4)
    piece_width = vit_width // pieces
    scalars = jnp.concatenate([index[:1], own_counts])
    hidden_rows, sent = attend(parts, places, scalars, mine, received, images, vit_out)
    received = [shift(sent[k - 1], k) for k in others]
    left, right = merge(parts, places, own_counts, hidden_rows, received, grads)
    main = places * piece_width
    if pieces > 1:
        merged = jnp.concatenate([left, right], axis=1)
        begin = (own_part % pieces) * piece_width
        taken = lax.dynamic_slice_in_dim(merged[:, :vit_width], begin, piece_width, 1)
        merged = jnp.concatenate([taken, merged[:, vit_width:]], axis=1)
        middle = min(merged.shape[1] // 2, main)
        left, right = merged[:, :middle], merged[:, middle:]
    left, right, key_source, gain_source, own_later = barrier(
        (left, right, key_weight, lang_norm_gain, own)
    )
    merged_all, grads, owners = gather_halves(left, right, main, own_later)

    part_features = width // parts
    own_start = own_later * feature_cols
    holder_part = own_start // part_features
    candidate = lax.dynamic_slice_in_dim(key_source, own_start % part_features, feature_cols, 0)
    key_rows = jnp.where(own_part == holder_part, candidate, jnp.zeros_like(candidate))
    held_by = [g * feature_cols // part_features for g in range(groups)]
    for k in others:
        pairs = [
            (held_by[g] * groups + g, (held_by[g] + k) % parts * groups + g) for g in range(groups)
        ]
        key_rows = key_rows + lax.ppermute(candidate, ("dp", "ctx"), pairs)
    own_gain = lax.dynamic_slice_in_dim(gain_source, own_start, feature_cols, 0).reshape(1, -1)

    def text_terms(blocks):
        rows = [blocks[0]] + [shift(blocks[k], k) for k in others]
        return dot(jnp.concatenate(rows, axis=0), key_weight)

    def text_return(terms):
        size = terms.shape[0] // parts
        return [shift(terms[k * size : (k + 1) * size].astype(BF16), -k) for k in others]

    early_terms = text_terms(text_blocks[0])

    grads = jnp.concatenate(grads, axis=0).reshape(groups, parts, capacity, key_width)
    block_owner = (owners[:, None] == group_index[None, :]).astype(jnp.int32)
    block_range = jnp.sum(block_owner[None] * target_range[:, None, :], axis=-1)
    routing = (block_range[:, :, None] == owners[None, None, :]).astype(BF16)
    grads = jnp.einsum("roi,irkw->orkw", routing, grads, preferred_element_type=F32).astype(BF16)
    weighted = (
        lax.dot_general(
            grads.reshape(-1, key_width),
            key_rows,
            (((1,), (1,)), ((), ())),
            preferred_element_type=F32,
        )
        * own_gain
    )

    embed_parts = [dot(rows, merger) for rows in merged_all]
    joined = jnp.concatenate(merged_all, axis=0)
    received = [[shift(part.astype(BF16), k) for k in others] for part in embed_parts]
    embedded, outgoing = features(
        parts, groups, owners, block_range[0], embed_parts, received, weighted, own_gain, key_rows
    )
    arrived = lax.all_to_all(outgoing, "ctx", 0, 0, tiled=True)
    late_terms = text_terms(text_blocks[1])
    returned = [text_return(early_terms), text_return(late_terms)]
    scales, grad_embedded = norm_scales(
        parts, groups, float(width), owners, arrived, embedded, weighted
    )
    merger_grad = lax.dot_general(
        joined, grad_embedded, (((0,), (0,)), ((), ())), preferred_element_type=F32
    )
    rotated = keys_out(
        parts,
        groups,
        index,
        image_grid,
        image_start,
        [early_terms, late_terms],
        returned,
        arrived,
        scales,
        cosine,
        sines,
    )
    return (rotated[None], merger_grad)


def solution(mesh):
    return jax.shard_map(
        on_device,
        mesh=mesh,
        in_specs=(
            P("dp", "ctx", None),
            P(),
            P("dp", None),
            P("dp", None),
            P("dp", "ctx"),
            P("dp", "ctx", None),
            P(),
            P("dp", None),
            P("dp", "ctx", None),
            P("dp", None, None),
            P("dp", None),
        ),
        out_specs=(P("dp", "ctx", None), P("dp", "ctx")),
        check_vma=False,
    )
```

```python
import math

import jax
import jax.numpy as jnp
from jax import lax
from jax.experimental import pallas as pl
from jax.experimental.pallas import tpu as pltpu
from jax.sharding import PartitionSpec as P


VHD = 80
HD = 128
EPS = 1e-06
THETA = 1000000.0
HIGHEST = lax.Precision.HIGHEST
BF16 = jnp.bfloat16
barrier = lax.optimization_barrier
F32 = jnp.float32


def layer_norm(values):
    average = jnp.mean(values, axis=-1, keepdims=True)
    centered = values - average
    variance = jnp.mean(centered * centered, axis=-1, keepdims=True)
    return centered * lax.rsqrt(variance + EPS)


def dot(a, b, **kw):
    return jnp.dot(a, b, preferred_element_type=F32, **kw)


def shift(x, k):
    size = lax.axis_size("dp")
    return lax.ppermute(x, "dp", [(i, (i + k) % size) for i in range(size)])


def gather_dp(x):
    return [x] + [shift(x, k) for k in range(1, lax.axis_size("dp"))]


def strides_of(size):
    return [1 << b for b in reversed(range(size.bit_length() - 1))]


def xor_gather(x, strides):
    size = lax.axis_size("ctx")
    pieces = [x]
    offsets = [[0]]
    for stride in strides:
        known = [o for piece in offsets for o in piece]
        joined = pieces[0] if len(pieces) == 1 else jnp.concatenate(pieces, axis=0)
        pieces.append(lax.ppermute(joined, "ctx", [(i, i ^ stride) for i in range(size)]))
        offsets.append([o ^ stride for o in known])
    return pieces, offsets


def gather_halves(left, right, main, own):
    size = lax.axis_size("ctx")
    middle, rows = left.shape[1], left.shape[0]
    if size & (size - 1) or size < 8:
        x = jnp.concatenate([left, right], axis=1)
        x = lax.all_gather(x, "ctx", axis=0, tiled=True)
        return [x[:, :main]], [x[:, main:]], jnp.arange(size, dtype=jnp.int32)
    strides = strides_of(size)
    lefts, offsets = xor_gather(left, strides[:-1])
    rights, others = xor_gather(right, strides[-2:-1] + strides[:-2])
    order = [o for piece in offsets for o in piece]
    found = {
        o: piece[j * rows : (j + 1) * rows]
        for piece, known in zip(rights, others)
        for j, o in enumerate(known)
    }
    rights = jnp.concatenate([found[o] for o in order], axis=0)
    low = jnp.concatenate([jnp.concatenate(lefts, axis=0), rights[:, : main - middle]], axis=1)
    rest = rights[:, main - middle :]
    low, own = barrier((low, own))
    pairs = [(i, i ^ 1) for i in range(size)]
    lows = [low, lax.ppermute(low, "ctx", pairs)]
    rests = [rest, lax.ppermute(rest, "ctx", pairs)]
    order = order + [o ^ 1 for o in order]
    return lows, rests, own ^ jnp.asarray(order, jnp.int32)


def find_image(own, tokens, grid_ref, start_ref, groups):
    zero = jnp.int32(0)
    first, cols, count, owner = zero, zero, zero, zero
    for o in range(groups):
        start = start_ref[0, o]
        here = (start >= own * tokens) & (start < (own + 1) * tokens)
        first = jnp.where(here, start, first)
        cols = jnp.where(here, grid_ref[1, o], cols)
        count = jnp.where(here, grid_ref[0, o] * grid_ref[1, o], count)
        owner = jnp.where(here, o, owner)
    return first, cols, count, owner


SMEM = pl.BlockSpec(memory_space=pltpu.SMEM)
VMEM = pl.BlockSpec(memory_space=pltpu.VMEM)


def call(kernel, outs, ins, scalars=0, scratch=()):
    return pl.pallas_call(
        kernel,
        out_shape=outs,
        in_specs=[SMEM] * scalars + [VMEM] * (len(ins) - scalars),
        out_specs=[VMEM] * len(outs),
        scratch_shapes=list(scratch),
    )(*ins)


def project(parts, index, images, gain, weight):
    rows, _ = images[0].shape
    depth, columns = weight.shape
    third = columns // 3
    block = third // parts

    def kernel(index_ref, *refs):
        image_refs = refs[:parts]
        gain_ref, weight_ref, mine_ref, sent_ref = refs[parts:]
        own = index_ref[0]
        pieces = []
        for r in range(parts):
            normed = layer_norm(image_refs[r][...].astype(F32)) * gain_ref[...]
            piece = normed[:, :depth]
            for b in range(1, parts):
                piece = jnp.where(own == b, normed[:, b * depth : (b + 1) * depth], piece)
            pieces.append(piece.astype(BF16))
        product = dot(jnp.concatenate(pieces, axis=0), weight_ref[...])
        for b in range(parts):
            heads = jnp.concatenate(
                [product[:, j * third + b * block : j * third + (b + 1) * block] for j in range(3)],
                axis=1,
            )

            @pl.when(own == b)
            def _():
                mine_ref[...] = heads.reshape(parts, rows, 3 * block)

            for k in range(1, parts):

                @pl.when((own + k) % parts == b)
                def _():
                    for r in range(parts):
                        sent_ref[k - 1, (r + k) % parts] = heads[r * rows : (r + 1) * rows].astype(
                            BF16
                        )

    return call(
        kernel,
        (
            jax.ShapeDtypeStruct((parts, rows, 3 * block), F32),
            jax.ShapeDtypeStruct((parts - 1, parts, rows, 3 * block), BF16),
        ),
        (index, *images, gain, weight),
        scalars=1,
    )


def attend(parts, places, scalars, mine, received, images, out_weight):
    rows, width = images[0].shape
    capacity = rows // 4
    block = out_weight.shape[0]
    heads = block // VHD
    taken = places * capacity

    def kernel(scalar_ref, *refs):
        mine_ref = refs[0]
        received_refs = refs[1:parts]
        image_refs = refs[parts : 2 * parts]
        weight_ref, hidden_ref, sent_ref, scratch = refs[2 * parts :]
        own = scalar_ref[0]
        lane = lax.broadcasted_iota(jnp.int32, (rows, block), 1)
        key_slot = lax.broadcasted_iota(jnp.int32, (heads * rows, rows), 1) % capacity
        attended = []
        for r in range(parts):
            total = mine_ref[r]
            for ref in received_refs:
                total = total + ref[r].astype(F32)
            total = total.astype(BF16)
            queries = total[:, :block]
            keys = total[:, block : 2 * block]
            contents = total[:, 2 * block :]
            in_head = [(lane >= h * VHD) & (lane < (h + 1) * VHD) for h in range(heads)]
            stacked = jnp.concatenate(
                [jnp.where(inside, queries, jnp.zeros_like(queries)) for inside in in_head], axis=0
            )
            scores = lax.dot_general(
                stacked, keys, (((1,), (1,)), ((), ())), preferred_element_type=F32
            ) / math.sqrt(VHD)
            alive = (key_slot < scalar_ref[1 + r]).astype(F32)
            weights = jnp.exp(scores) * alive
            probability = (weights / jnp.sum(weights, axis=-1, keepdims=True)).astype(BF16)
            spread = dot(probability, contents)
            picked = jnp.where(in_head[0], spread[:rows], 0.0)
            for h in range(1, heads):
                picked = picked + jnp.where(in_head[h], spread[h * rows : (h + 1) * rows], 0.0)
            attended.append(picked.astype(BF16))
        product = dot(jnp.concatenate(attended, axis=0), weight_ref[...])
        scratch[...] = product.reshape(parts, rows, width)

        def start(index):
            return pl.multiple_of((index * 4 // parts) * capacity, capacity)

        for r in range(parts):
            at = pl.ds(start(own), taken)
            hidden_ref[r] = scratch[r, at, :] + image_refs[r][at, :].astype(F32)
            for k in range(1, parts):
                at = pl.ds(start((own + k) % parts), taken)
                sent_ref[k - 1, (r + k) % parts] = scratch[r, at, :].astype(BF16)

    return call(
        kernel,
        (
            jax.ShapeDtypeStruct((parts, taken, width), F32),
            jax.ShapeDtypeStruct((parts - 1, parts, taken, width), BF16),
        ),
        (scalars, mine, *received, *images, out_weight),
        scalars=1,
        scratch=[pltpu.VMEM((parts, rows, width), F32)],
    )


def features(parts, groups, owners, holders, own_parts, received, weighted, gain, key_rows):
    total = sum(p.shape[0] for p in own_parts)
    columns = own_parts[0].shape[1]
    rows = total // groups
    capacity = rows // parts
    key_width = key_rows.shape[1]
    chunks = len(own_parts)
    per_chunk = groups // chunks
    sum_rows = -(-6 * (total // key_width) // 8) * 8
    flat = [r for group in received for r in group]

    def kernel(owner_ref, holder_ref, *refs):
        part_refs = refs[:chunks]
        received_refs = refs[chunks : chunks + len(flat)]
        weighted_ref, gain_ref, key_ref, embed_ref, keys_ref, squared, multiplied = refs[
            chunks + len(flat) :
        ]
        picked = []
        for i in range(groups):
            chunk, base = i // per_chunk, (i % per_chunk) * rows
            block = part_refs[chunk][base : base + rows, :]
            for k in range(1, parts):
                ref = received_refs[chunk * (parts - 1) + k - 1]
                block = block + jnp.concatenate(
                    [
                        ref[pl.ds(base + (r - k) % parts * capacity, capacity), :].astype(F32)
                        for r in range(parts)
                    ],
                    axis=0,
                )
            block = block.astype(BF16)
            picked.append((block[:capacity].astype(F32) * gain_ref[...]).astype(BF16))
            embed_ref[pl.ds(i * rows, rows), :] = block
            values = block.astype(F32)
            at = pl.ds(pl.multiple_of(owner_ref[i] * rows, rows), rows)
            squared[at, :] = values * values
            multiplied[at, :] = values * weighted_ref[pl.ds(i * rows, rows), :]
        ones = jnp.ones((8, columns), F32)
        both = [
            lax.dot_general(
                ones,
                ref[...],
                (((1,), (1,)), ((), ())),
                precision=HIGHEST,
                preferred_element_type=F32,
            )[0:1]
            for ref in (squared, multiplied)
        ]
        lines = []
        for _ in range(3):
            rounded = [v.astype(BF16).astype(F32) for v in both]
            both = [v - w for v, w in zip(both, rounded)]
            for v in rounded:
                lines += [v[:, j : j + key_width] for j in range(0, total, key_width)]
        lines += [jnp.zeros_like(lines[0])] * (sum_rows - len(lines))
        lines = jnp.concatenate(lines, axis=0).astype(BF16)
        terms = dot(jnp.concatenate(picked, axis=0), key_ref[...]).astype(BF16)
        for i in range(groups):
            keys_ref[holder_ref[i], 0:capacity] = terms[i * capacity : (i + 1) * capacity]
            keys_ref[i, capacity:] = lines

    return call(
        kernel,
        (
            jax.ShapeDtypeStruct((total, columns), BF16),
            jax.ShapeDtypeStruct((groups, capacity + sum_rows, key_width), BF16),
        ),
        (owners, holders, *own_parts, *flat, weighted, gain, key_rows),
        scalars=2,
        scratch=[pltpu.VMEM((total, columns), F32), pltpu.VMEM((total, columns), F32)],
    )


def norm_scales(parts, groups, width, owners, arrived, embedded, weighted):
    total, columns = embedded.shape
    rows = total // groups
    capacity = rows // parts
    lines = total // arrived.shape[2]

    def kernel(owner_ref, sums_ref, embed_ref, weighted_ref, scale_ref, grad_ref, turned):
        summed = jnp.sum(sums_ref[:, capacity:, :].astype(F32), axis=0)

        def whole(q):
            pieces = []
            for j in range(lines):
                at = [(2 * p + q) * lines + j for p in range(3)]
                pieces.append(sum(summed[r : r + 1] for r in at))
            return jnp.concatenate(pieces, axis=1)

        scale = lax.rsqrt(whole(0) / width + EPS)
        slope = scale**3 * whole(1) / width
        line = lax.broadcasted_iota(jnp.int32, (8, total), 0)
        both = jnp.where(line == 0, scale, slope)
        scale_ref[...] = both
        turned[...] = jnp.transpose(both)
        for i in range(groups):
            at = pl.ds(i * rows, rows)
            both = turned[pl.ds(pl.multiple_of(owner_ref[i] * rows, rows), rows), :]
            grad = both[:, 0:1] * weighted_ref[at, :] - embed_ref[at, :].astype(F32) * both[:, 1:2]
            grad_ref[at, :] = grad.astype(BF16)

    return call(
        kernel,
        (jax.ShapeDtypeStruct((8, total), F32), jax.ShapeDtypeStruct((total, columns), BF16)),
        (owners, arrived, embedded, weighted),
        scalars=1,
        scratch=[pltpu.VMEM((total, 8), F32)],
    )


def merge(parts, places, counts, hidden, received, extras):
    taken, width = hidden.shape[1:]
    capacity = taken // places
    main = places * width
    middle = (main + extras[0].shape[1]) // 256 * 128
    rest = main + extras[0].shape[1] - middle
    count = len(received)

    def kernel(count_ref, *refs):
        hidden_ref, received_refs = refs[0], refs[1 : 1 + count]
        extra_refs, left_ref, right_ref = refs[1 + count : -2], refs[-2], refs[-1]

        def put(rows, column, values):
            split = min(max(middle - column, 0), values.shape[1])
            if split:
                left_ref[rows, column : column + split] = values[:, :split]
            if split < values.shape[1]:
                begin = column + split - middle
                right_ref[rows, begin : begin + values.shape[1] - split] = values[:, split:]

        slot = lax.broadcasted_iota(jnp.int32, (capacity, width), 0)
        for r in range(parts):
            rows = pl.ds(r * capacity, capacity)
            total = hidden_ref[r]
            for ref in received_refs:
                total = total + ref[r].astype(F32)
            normed = layer_norm(total).astype(BF16)
            for p in range(places):
                kept = normed[p * capacity : (p + 1) * capacity]
                put(rows, p * width, jnp.where(slot < count_ref[r], kept, jnp.zeros_like(kept)))
            put(rows, main, extra_refs[r][...])

    return call(
        kernel,
        (
            jax.ShapeDtypeStruct((parts * capacity, middle), BF16),
            jax.ShapeDtypeStruct((parts * capacity, rest), BF16),
        ),
        (counts, hidden, *received, *extras),
        scalars=1,
    )


def angle_table(tokens, groups, capacity, index, grid, start):
    half = HD // 2
    first_cut = HD // 8
    second_cut = first_cut + 3 * HD // 16
    inverse = THETA ** (-(2.0 * (jnp.arange(HD, dtype=jnp.int32) % half).astype(F32)) / HD)

    def kernel(index_ref, grid_ref, start_ref, inverse_ref, out_ref):
        own = index_ref[1]
        first, cols, count, _ = find_image(own, tokens, grid_ref, start_ref, groups)
        line = lax.broadcasted_iota(jnp.int32, (tokens, HD), 0) + own * tokens
        frequency = lax.broadcasted_iota(jnp.int32, (tokens, HD), 1) % half
        inner = line - first
        row = jnp.zeros_like(inner)
        for j in range(1, capacity):
            row = row + (inner >= j * cols).astype(jnp.int32)
        offset = jnp.where(frequency < second_cut, row, inner - row * cols)
        offset = jnp.where(frequency < first_cut, 0, offset)
        inside = (inner >= 0) & (inner < count)
        chosen = jnp.where(inside, first + offset, line)
        out_ref[...] = chosen.astype(F32) * inverse_ref[...]

    return call(
        kernel,
        (jax.ShapeDtypeStruct((tokens, HD), F32),),
        (index, grid, start, inverse.reshape(1, -1)),
        scalars=3,
    )[0]


def place_rows(tokens, own, first, count, shape, axis):
    token = lax.broadcasted_iota(jnp.int32, shape, axis)
    slot = lax.broadcasted_iota(jnp.int32, shape, 1 - axis)
    return ((token + own * tokens - first == slot) & (slot < count)).astype(F32)


def turn(values, cosine, sines):
    heads = []
    for h in range(values.shape[1] // HD):
        head = values[:, h * HD : (h + 1) * HD]
        heads.append(head * cosine + pltpu.roll(head, HD // 2, 1) * sines)
    return jnp.concatenate(heads, axis=1)


def image_grads(tokens, groups, capacity, index, grid, start, cotangent, cosine, sines):
    width = cotangent.shape[1]

    def kernel(index_ref, grid_ref, start_ref, cotangent_ref, cosine_ref, sine_ref, out_ref):
        own = index_ref[1]
        first, _, count, _ = find_image(own, tokens, grid_ref, start_ref, groups)
        lane = lax.broadcasted_iota(jnp.int32, (tokens, HD), 1)
        signed = jnp.where(lane < HD // 2, sine_ref[...], -sine_ref[...])
        grad = turn(cotangent_ref[...].astype(F32), cosine_ref[...], signed)
        chosen = place_rows(tokens, own, first, count, (capacity, tokens), 1)
        out_ref[...] = dot(chosen, grad, precision=HIGHEST).astype(BF16)

    return call(
        kernel,
        (jax.ShapeDtypeStruct((capacity, width), BF16),),
        (index, grid, start, cotangent, cosine, sines),
        scalars=3,
    )[0]


def keys_out(parts, groups, index, grid, start, text_keys, returned, arrived, scales, cosine, sines):
    tokens, width = cosine.shape[0], text_keys[0].shape[1]
    total = scales.shape[1]
    capacity = total // (parts * groups)
    chunks = len(text_keys)
    sizes = [t.shape[0] // parts for t in text_keys]
    flat = [r for group in returned for r in group]

    def kernel(index_ref, grid_ref, start_ref, *refs):
        text_refs = refs[:chunks]
        returned_refs = refs[chunks : chunks + len(flat)]
        arrived_ref, scale_ref, cosine_ref, sine_ref, out_ref = refs[chunks + len(flat) :]
        own = index_ref[1]
        first, _, count, owner = find_image(own, tokens, grid_ref, start_ref, groups)
        shape = (capacity, total)
        lane = lax.broadcasted_iota(jnp.int32, shape, 1)
        slot = lax.broadcasted_iota(jnp.int32, shape, 0)
        wanted = lane == owner * (parts * capacity) + slot
        scale = jnp.sum(jnp.where(wanted, scale_ref[0:1, :], 0.0), axis=-1, keepdims=True)
        image = jnp.sum(arrived_ref[:, 0:capacity, :].astype(F32), axis=0) * scale
        chosen = place_rows(tokens, own, first, count, (tokens, capacity), 0)
        placed = dot(chosen, image, precision=HIGHEST)
        token = lax.broadcasted_iota(jnp.int32, (tokens, width), 0) + own * tokens
        inside = (token >= first) & (token < first + count)
        lane = lax.broadcasted_iota(jnp.int32, (tokens, HD), 1)
        signed = jnp.where(lane < HD // 2, -sine_ref[...], sine_ref[...])
        rows = []
        for j in range(chunks):
            part = text_refs[j][0 : sizes[j], :]
            for k in range(parts - 1):
                part = part + returned_refs[j * (parts - 1) + k][...].astype(F32)
            rows.append(part)
        keys = jnp.where(inside, placed, jnp.concatenate(rows, axis=0))
        out_ref[...] = turn(keys, cosine_ref[...], signed).astype(BF16)

    return call(
        kernel,
        (jax.ShapeDtypeStruct((tokens, width), BF16),),
        (index, grid, start, *text_keys, *flat, arrived, scales, cosine, sines),
        scalars=3,
    )[0]


def text_norm(parts, sizes, index, text, gain):
    tokens, width = text.shape
    step = math.gcd(32, *sizes)
    block = width // parts
    steps = [size // step for size in sizes]
    begins = [sum(steps[:j]) for j in range(len(steps))]

    def kernel(index_ref, text_ref, gain_ref, *refs):
        out_refs, scratch = refs[:-1], refs[-1]
        values = text_ref[...].astype(F32)
        scale = lax.rsqrt(jnp.mean(values * values, axis=-1, keepdims=True) + EPS)
        scratch[...] = (values * scale * gain_ref[...]).astype(BF16)
        now = pl.program_id(0)
        for j in range(len(sizes)):

            @pl.when((now >= begins[j]) & (now < begins[j] + steps[j]))
            def _():
                for k in range(parts):
                    start = pl.multiple_of((index_ref[0] + k) % parts * block, block)
                    out_refs[j * parts + k][...] = scratch[:, pl.ds(start, block)]

    def place(j):
        return lambda g: (jnp.clip(g - begins[j], 0, steps[j] - 1), 0)

    flat = pl.pallas_call(
        kernel,
        grid=(tokens // step,),
        out_shape=[jax.ShapeDtypeStruct((size, block), BF16) for size in sizes for _ in range(parts)],
        in_specs=[
            SMEM,
            pl.BlockSpec((step, width), lambda g: (g, 0)),
            pl.BlockSpec((1, width), lambda g: (0, 0)),
        ],
        out_specs=[
            pl.BlockSpec((step, block), place(j)) for j in range(len(sizes)) for _ in range(parts)
        ],
        scratch_shapes=[pltpu.VMEM((step, width), BF16)],
        name="text_norm",
    )(index, text, gain)
    return [flat[j * parts : (j + 1) * parts] for j in range(len(sizes))]


def on_device(
    patches,
    vit_norm_gain,
    vit_qkv,
    vit_out,
    merger,
    text_embed,
    lang_norm_gain,
    key_weight,
    key_cotangent,
    image_grid,
    image_start,
):
    parts = lax.axis_size("dp")
    groups = lax.axis_size("ctx")
    own_part = lax.axis_index("dp")
    own = lax.axis_index("ctx")
    tokens, width = text_embed.shape[1:]
    vit_width = patches.shape[2]
    capacity = patches.shape[1] // 4
    key_width = key_weight.shape[1]
    feature_cols = merger.shape[1]
    gain_line = lang_norm_gain.reshape(1, -1)
    index = jnp.stack([own_part, own]).astype(jnp.int32)
    others = range(1, parts)

    row = jnp.arange(4 * capacity, dtype=jnp.int32)
    source_row = (row % capacity) * 4 + row // capacity
    order_rows = (source_row[:, None] == row[None, :]).astype(BF16)
    images = gather_dp(dot(order_rows, patches[0]).astype(BF16))

    info = jnp.concatenate([image_grid[0].T, image_start], axis=0)
    infos = jnp.stack(gather_dp(info))
    counts = infos[:, 0] * infos[:, 1]
    target_range = infos[:, 2] // tokens
    group_index = jnp.arange(groups, dtype=jnp.int32)
    own_counts = jnp.sum(jnp.where(group_index[None] == own, counts, 0), axis=1)

    sizes = [tokens - tokens // 4, tokens // 4]
    text_blocks = text_norm(parts, sizes, index, text_embed[0], gain_line)

    mine, sent = project(parts, index, images, vit_norm_gain.reshape(1, -1), vit_qkv)

    sent, grid, start = barrier((sent, image_grid[0].T, image_start))
    received = [shift(sent[k - 1], k) for k in others]
    angles = angle_table(tokens, groups, capacity, index, grid, start)
    cosine, sines = jnp.cos(angles), jnp.sin(angles)
    grads = image_grads(
        tokens, groups, capacity, index, grid, start, key_cotangent[0], cosine, sines
    )
    grads = gather_dp(grads)

    places = max(1, 4 // parts)
    pieces = max(1, parts // 4)
    piece_width = vit_width // pieces
    scalars = jnp.concatenate([index[:1], own_counts])
    hidden_rows, sent = attend(parts, places, scalars, mine, received, images, vit_out)
    received = [shift(sent[k - 1], k) for k in others]
    left, right = merge(parts, places, own_counts, hidden_rows, received, grads)
    main = places * piece_width
    if pieces > 1:
        merged = jnp.concatenate([left, right], axis=1)
        begin = (own_part % pieces) * piece_width
        taken = lax.dynamic_slice_in_dim(merged[:, :vit_width], begin, piece_width, 1)
        merged = jnp.concatenate([taken, merged[:, vit_width:]], axis=1)
        middle = min(merged.shape[1] // 2, main)
        left, right = merged[:, :middle], merged[:, middle:]
    left, right, key_source, gain_source, own_later = barrier(
        (left, right, key_weight, lang_norm_gain, own)
    )
    merged_all, grads, owners = gather_halves(left, right, main, own_later)

    part_features = width // parts
    own_start = own_later * feature_cols
    holder_part = own_start // part_features
    candidate = lax.dynamic_slice_in_dim(key_source, own_start % part_features, feature_cols, 0)
    key_rows = jnp.where(own_part == holder_part, candidate, jnp.zeros_like(candidate))
    held_by = [g * feature_cols // part_features for g in range(groups)]
    for k in others:
        pairs = [
            (held_by[g] * groups + g, (held_by[g] + k) % parts * groups + g) for g in range(groups)
        ]
        key_rows = key_rows + lax.ppermute(candidate, ("dp", "ctx"), pairs)
    own_gain = lax.dynamic_slice_in_dim(gain_source, own_start, feature_cols, 0).reshape(1, -1)

    def text_terms(blocks):
        rows = [blocks[0]] + [shift(blocks[k], k) for k in others]
        return dot(jnp.concatenate(rows, axis=0), key_weight)

    def text_return(terms):
        size = terms.shape[0] // parts
        return [shift(terms[k * size : (k + 1) * size].astype(BF16), -k) for k in others]

    early_terms = text_terms(text_blocks[0])

    grads = jnp.concatenate(grads, axis=0).reshape(groups, parts, capacity, key_width)
    block_owner = (owners[:, None] == group_index[None, :]).astype(jnp.int32)
    block_range = jnp.sum(block_owner[None] * target_range[:, None, :], axis=-1)
    routing = (block_range[:, :, None] == owners[None, None, :]).astype(BF16)
    grads = jnp.einsum("roi,irkw->orkw", routing, grads, preferred_element_type=F32).astype(BF16)
    weighted = (
        lax.dot_general(
            grads.reshape(-1, key_width),
            key_rows,
            (((1,), (1,)), ((), ())),
            preferred_element_type=F32,
        )
        * own_gain
    )

    embed_parts = [dot(rows, merger) for rows in merged_all]
    joined = jnp.concatenate(merged_all, axis=0)
    received = [[shift(part.astype(BF16), k) for k in others] for part in embed_parts]
    embedded, outgoing = features(
        parts, groups, owners, block_range[0], embed_parts, received, weighted, own_gain, key_rows
    )
    arrived = lax.all_to_all(outgoing, "ctx", 0, 0, tiled=True)
    late_terms = text_terms(text_blocks[1])
    returned = [text_return(early_terms), text_return(late_terms)]
    scales, grad_embedded = norm_scales(
        parts, groups, float(width), owners, arrived, embedded, weighted
    )
    merger_grad = lax.dot_general(
        joined, grad_embedded, (((0,), (0,)), ((), ())), preferred_element_type=F32
    )
    rotated = keys_out(
        parts,
        groups,
        index,
        image_grid[0].T,
        image_start,
        [early_terms, late_terms],
        returned,
        arrived,
        scales,
        cosine,
        sines,
    )
    return (rotated[None], merger_grad)


def solution(mesh):
    return jax.shard_map(
        on_device,
        mesh=mesh,
        in_specs=(
            P("dp", "ctx", None),
            P(),
            P("dp", None),
            P("dp", None),
            P("dp", "ctx"),
            P("dp", "ctx", None),
            P(),
            P("dp", None),
            P("dp", "ctx", None),
            P("dp", None, None),
            P("dp", None),
        ),
        out_specs=(P("dp", "ctx", None), P("dp", "ctx")),
        check_vma=False,
    )
```
